8 devices in a mesh: my: 4 (over z, y, x), mx: 2 (over core).
Axes of the slice: x: 2, y: 2, z: 1, core: 2. Of those that a mesh axis runs over, the one named last changes fastest.
Arguments:
- x_in: bfloat16 [384, 5120], P(None, 'mx')
- seq_lens: int32 [384], P('mx')
- gain_attn: bfloat16 [5120], P('mx')
- gain_mlp: bfloat16 [5120], P('mx')
- w_q: bfloat16 [5120, 5120], P('mx', 'my')
- b_q: bfloat16 [5120], P('my')
- w_k: bfloat16 [5120, 1024], P('mx', 'my')
- b_k: bfloat16 [1024], P('my')
- w_v: bfloat16 [5120, 1024], P('mx', 'my')
- b_v: bfloat16 [1024], P('my')
- w_o: bfloat16 [5120, 5120], P('my', 'mx')
- w_gate: bfloat16 [5120, 13824], P('mx', 'my')
- w_up: bfloat16 [5120, 13824], P('mx', 'my')
- w_down: bfloat16 [13824, 5120], P('my', 'mx')
- k_cache: bfloat16 [384, 256, 8, 128], P('mx', None, 'my')
- v_cache: bfloat16 [384, 256, 8, 128], P('mx', None, 'my')
Outputs:
- output 1: bfloat16 [384, 5120], P(None, 'mx')
- output 2: bfloat16 [384, 256, 8, 128], P('mx', None, 'my')
- output 3: bfloat16 [384, 256, 8, 128], P('mx', None, 'my')
All inputs are finite; a program needn't handle non-finite values.
Results may differ from the reference program's by a relative error of at most 0.0165212.
Values are sent between devices in bfloat16 or wider.
A program may use at most 1 GiB of HBM per device.

```python
import jax
import jax.numpy as jnp
from jax import lax

D = 5120
HEADS = 40
KV_HEADS = 8
HEAD = 128
FF = 13824
BATCH = 384
SEQ = 256
NORM_EPS = 1e-6
ROPE_THETA = 1000000.0
GROUP = HEADS // KV_HEADS


def setup_inputs(seed: int = 0) -> dict:
    key_list = jax.random.split(jax.random.key(seed), 17)
    q_width = HEADS * HEAD
    kv_width = KV_HEADS * HEAD
    cache_shape = (BATCH, SEQ, KV_HEADS, HEAD)

    def normal(key_index, shape, scale, offset=0.0):
        samples = jax.random.normal(key_list[key_index], shape, jnp.float32)
        return (offset + scale * samples).astype(jnp.bfloat16)

    lens_draw = jax.random.randint(key_list[0], (BATCH,), 0, SEQ)
    full_row = jax.random.randint(key_list[1], (), 0, BATCH)
    seq_lens = jnp.where(jnp.arange(BATCH) == full_row, SEQ - 1, lens_draw).astype(jnp.int32)
    return {
        "x_in": normal(2, (BATCH, D), 1.0),
        "seq_lens": seq_lens,
        "gain_attn": normal(3, (D,), 0.3, 1.0),
        "gain_mlp": normal(4, (D,), 0.3, 1.0),
        "w_q": normal(5, (D, q_width), 2.0 * D ** -0.5),
        "b_q": normal(6, (q_width,), 1.0),
        "w_k": normal(7, (D, kv_width), D ** -0.5),
        "b_k": normal(8, (kv_width,), 1.0),
        "w_v": normal(9, (D, kv_width), D ** -0.5),
        "b_v": normal(10, (kv_width,), 1.0),
        "w_o": normal(11, (q_width, D), q_width ** -0.5),
        "w_gate": normal(12, (D, FF), D ** -0.5),
        "w_up": normal(13, (D, FF), D ** -0.5),
        "w_down": normal(14, (FF, D), FF ** -0.5),
        "k_cache": normal(15, cache_shape, 1.0),
        "v_cache": normal(16, cache_shape, 1.0),
    }


def rms_norm(rows_in, gain_vec):
    rows_f32 = rows_in.astype(jnp.float32)
    mean_sq = jnp.mean(rows_f32 * rows_f32, axis=-1, keepdims=True)
    return (rows_f32 * lax.rsqrt(mean_sq + NORM_EPS) * gain_vec.astype(jnp.float32)).astype(jnp.bfloat16)


def apply_rotary(vectors, positions):
    half_dim = HEAD // 2
    inv_freq = ROPE_THETA ** (-2.0 * jnp.arange(half_dim, dtype=jnp.float32) / HEAD)
    angles = positions.astype(jnp.float32)[:, None, None] * inv_freq
    cos_tab = jnp.cos(angles)
    sin_tab = jnp.sin(angles)
    lower_half = vectors[..., :half_dim]
    upper_half = vectors[..., half_dim:]
    return jnp.concatenate([lower_half * cos_tab - upper_half * sin_tab, upper_half * cos_tab + lower_half * sin_tab], axis=-1)


def attend_one(row_inputs):
    q_row, k_rows, v_rows, length = row_inputs
    q_grouped = q_row.reshape(KV_HEADS, GROUP, HEAD).astype(jnp.float32)
    scores = jnp.einsum("kgd,skd->kgs", q_grouped, k_rows.astype(jnp.float32)) * HEAD ** -0.5
    visible = (jnp.arange(SEQ) <= length)[None, None, :]
    scores = jnp.where(visible, scores, -jnp.inf)
    weights = jnp.exp(scores - jnp.max(scores, axis=-1, keepdims=True))
    weight_sum = jnp.sum(weights, axis=-1, keepdims=True)
    weighted = jnp.einsum("kgs,skd->kgd", weights.astype(jnp.bfloat16).astype(jnp.float32), v_rows.astype(jnp.float32))
    return (weighted / weight_sum).astype(jnp.bfloat16).reshape(HEADS * HEAD)


def reference(x_in, seq_lens, gain_attn, gain_mlp, w_q, b_q, w_k, b_k, w_v, b_v, w_o, w_gate, w_up, w_down, k_cache, v_cache):
    normed = rms_norm(x_in, gain_attn)
    q_vals = jnp.dot(normed, w_q, preferred_element_type=jnp.float32) + b_q.astype(jnp.float32)
    k_vals = jnp.dot(normed, w_k, preferred_element_type=jnp.float32) + b_k.astype(jnp.float32)
    v_vals = jnp.dot(normed, w_v, preferred_element_type=jnp.float32) + b_v.astype(jnp.float32)
    q_rot = apply_rotary(q_vals.reshape(BATCH, HEADS, HEAD), seq_lens).astype(jnp.bfloat16)
    k_rot = apply_rotary(k_vals.reshape(BATCH, KV_HEADS, HEAD), seq_lens).astype(jnp.bfloat16)
    v_new = v_vals.reshape(BATCH, KV_HEADS, HEAD).astype(jnp.bfloat16)
    at_slot = (jnp.arange(SEQ)[None, :] == seq_lens[:, None])[:, :, None, None]
    k_cache_out = jnp.where(at_slot, k_rot[:, None], k_cache)
    v_cache_out = jnp.where(at_slot, v_new[:, None], v_cache)
    attn_rows = lax.map(attend_one, (q_rot, k_cache_out, v_cache_out, seq_lens))
    x_mid = (x_in.astype(jnp.float32) + jnp.dot(attn_rows, w_o, preferred_element_type=jnp.float32)).astype(jnp.bfloat16)
    normed_mlp = rms_norm(x_mid, gain_mlp)
    gate_proj = jnp.dot(normed_mlp, w_gate, preferred_element_type=jnp.float32)
    up_proj = jnp.dot(normed_mlp, w_up, preferred_element_type=jnp.float32)
    hidden_act = (jax.nn.silu(gate_proj) * up_proj).astype(jnp.bfloat16)
    x_out = (x_mid.astype(jnp.float32) + jnp.dot(hidden_act, w_down, preferred_element_type=jnp.float32)).astype(jnp.bfloat16)
    return (x_out, k_cache_out, v_cache_out)
```

```python
import jax
import jax.numpy as jnp
from jax import lax
from jax.experimental import pallas as pl
from jax.experimental.pallas import tpu as pltpu
from jax.sharding import PartitionSpec as P

HEAD = 128
NORM_EPS = 1e-6
ROPE_THETA = 1000000.0
SLOT_ROWS = 8
SLOTS = 8
AHEAD = 6
PAD_HEADS = 16


def attend_kernel(lens, q_ref, kn_ref, vn_ref, kc, vc, ko, vo, out_ref, kbuf, vbuf, qs, os, sems):
    rows = q_ref.shape[0]
    heads = q_ref.shape[1] // HEAD
    flat = kbuf.shape[2]
    blocks = rows // SLOT_ROWS

    def moves(block, slot, inward):
        part = pl.ds(block * SLOT_ROWS, SLOT_ROWS)
        if inward:
            return (pltpu.make_async_copy(kc.at[part], kbuf.at[slot], sems.at[0, slot]),
                    pltpu.make_async_copy(vc.at[part], vbuf.at[slot], sems.at[1, slot]))
        return (pltpu.make_async_copy(kbuf.at[slot], ko.at[part], sems.at[2, slot]),
                pltpu.make_async_copy(vbuf.at[slot], vo.at[part], sems.at[3, slot]))

    for block in range(AHEAD):
        for move in moves(block, block, True):
            move.start()
    qs[...] = jnp.zeros_like(qs)

    tile_row = lax.broadcasted_iota(jnp.int32, (PAD_HEADS, HEAD), 0)
    pair_row = lax.broadcasted_iota(jnp.int32, (2 * PAD_HEADS, flat), 0)
    col = lax.broadcasted_iota(jnp.int32, (2 * PAD_HEADS, flat), 1)
    second = pair_row >= PAD_HEADS
    head_of_row = jnp.where(pair_row % PAD_HEADS >= heads // 2, 1, 0)
    col_pos = jnp.where(col % 2 == head_of_row, col // 2, jnp.int32(1 << 20))
    zeros = jnp.zeros((PAD_HEADS, HEAD), jnp.bfloat16)

    def put_row(buf, slot, j, pos, new8):
        base = pl.multiple_of((2 * pos) // 16 * 16, 16)
        off = 2 * pos - base
        tile = buf[slot, j, pl.ds(base, 16), :]
        first = jnp.broadcast_to(new8[j:j + 1, :HEAD], (16, HEAD)).astype(jnp.bfloat16)
        other = jnp.broadcast_to(new8[j:j + 1, HEAD:], (16, HEAD)).astype(jnp.bfloat16)
        tile = jnp.where(tile_row == off, first, jnp.where(tile_row == off + 1, other, tile))
        buf[slot, j, pl.ds(base, 16), :] = tile

    @pl.loop(0, blocks // 2)
    def _(step):
        for half in range(2):
            block = step * 2 + half
            slot = lax.rem(block, SLOTS)
            for move in moves(block, slot, True):
                move.wait()
            rows8 = pl.ds(pl.multiple_of(block * SLOT_ROWS, SLOT_ROWS), SLOT_ROWS)
            kn8, vn8 = kn_ref[rows8, :], vn_ref[rows8, :]
            for h in range(heads):
                qs[pl.ds(h, SLOT_ROWS, stride=PAD_HEADS), :] = q_ref[rows8, h * HEAD:(h + 1) * HEAD]
            for j in range(SLOT_ROWS):
                b = block * SLOT_ROWS + j
                put_row(kbuf, slot, j, lens[b], kn8)
                put_row(vbuf, slot, j, lens[b], vn8)
            pairs = range(0, SLOT_ROWS, 2)
            scores = []
            for j in pairs:
                q0 = qs[j * PAD_HEADS:(j + 1) * PAD_HEADS, :].astype(jnp.bfloat16)
                q1 = qs[(j + 1) * PAD_HEADS:(j + 2) * PAD_HEADS, :].astype(jnp.bfloat16)
                qp = jnp.concatenate([jnp.concatenate([q0, zeros], axis=1), jnp.concatenate([zeros, q1], axis=1)], axis=0)
                kp = jnp.concatenate([kbuf[slot, j], kbuf[slot, j + 1]], axis=1)
                scores.append(lax.dot_general(qp, kp, (((1,), (1,)), ((), ())), preferred_element_type=jnp.float32))
            probs = []
            for i, j in enumerate(pairs):
                b = block * SLOT_ROWS + j
                limit = jnp.where(second, lens[b + 1], lens[b])
                s = jnp.where(col_pos <= limit, scores[i] * HEAD ** -0.5, -jnp.inf)
                e = jnp.exp(s - jnp.max(s, axis=-1, keepdims=True))
                probs.append((e.astype(jnp.bfloat16), jnp.sum(e, axis=-1, keepdims=True)))
            for i, j in enumerate(pairs):
                e, total = probs[i]
                vp = jnp.concatenate([vbuf[slot, j], vbuf[slot, j + 1]], axis=1)
                o = jnp.dot(e, vp, preferred_element_type=jnp.float32)
                at = (half * SLOT_ROWS + j) * PAD_HEADS
                os[at:at + PAD_HEADS, :] = o[:PAD_HEADS, :HEAD] / total[:PAD_HEADS]
                os[at + PAD_HEADS:at + 2 * PAD_HEADS, :] = o[PAD_HEADS:, HEAD:] / total[PAD_HEADS:]
            for move in moves(block, slot, False):
                move.start()

            @pl.when(block + AHEAD < blocks)
            def _():
                later = lax.rem(block + AHEAD, SLOTS)

                @pl.when(block + AHEAD >= SLOTS)
                def _():
                    for move in moves(block + AHEAD - SLOTS, later, False):
                        move.wait()
                for move in moves(block + AHEAD, later, True):
                    move.start()
        for h in range(heads):
            out_ref[pl.ds(pl.multiple_of(step * 16, 16), 16), h * HEAD:(h + 1) * HEAD] = os[pl.ds(h, 16, stride=PAD_HEADS), :].astype(jnp.bfloat16)

    for block in range(blocks - SLOTS, blocks):
        for move in moves(block, block % SLOTS, False):
            move.wait()


def attend(lens, q, k_new, v_new, k_cache, v_cache):
    rows, seq, kv, _ = k_cache.shape
    flat = seq * kv
    kc = k_cache.reshape(rows, flat, HEAD)
    vc = v_cache.reshape(rows, flat, HEAD)
    whole = pl.BlockSpec(memory_space=pltpu.VMEM)
    hbm = pl.BlockSpec(memory_space=pltpu.HBM)
    ko, vo, out = pl.pallas_call(
        attend_kernel,
        out_shape=(jax.ShapeDtypeStruct(kc.shape, kc.dtype), jax.ShapeDtypeStruct(vc.shape, vc.dtype), jax.ShapeDtypeStruct(q.shape, jnp.bfloat16)),
        in_specs=[pl.BlockSpec(memory_space=pltpu.SMEM), whole, whole, whole, hbm, hbm],
        out_specs=(hbm, hbm, whole),
        scratch_shapes=[
            pltpu.VMEM((SLOTS, SLOT_ROWS, flat, HEAD), jnp.bfloat16),
            pltpu.VMEM((SLOTS, SLOT_ROWS, flat, HEAD), jnp.bfloat16),
            pltpu.VMEM((SLOT_ROWS * PAD_HEADS, HEAD), jnp.float32),
            pltpu.VMEM((2 * SLOT_ROWS * PAD_HEADS, HEAD), jnp.float32),
            pltpu.SemaphoreType.DMA((4, SLOTS)),
        ],
        compiler_params=pltpu.CompilerParams(vmem_limit_bytes=40 << 20),
        name="attend",
    )(lens, q, k_new, v_new, kc, vc)
    return ko.reshape(k_cache.shape), vo.reshape(v_cache.shape), out


def rotate(cols, cos_tab, sin_tab):
    rows, width = cols.shape
    heads = cols.reshape(rows, width // HEAD, HEAD)
    lower, upper = heads[..., :HEAD // 2], heads[..., HEAD // 2:]
    out = jnp.concatenate([lower * cos_tab - upper * sin_tab, upper * cos_tab + lower * sin_tab], axis=-1)
    return out.astype(jnp.bfloat16).astype(jnp.float32).reshape(rows, width)


def solution(mesh):
    mx_size = mesh.shape["mx"]
    act_spec = P(None, "mx")
    cache_spec = P("mx", None, "my", None)
    in_specs = (act_spec, P("mx"), P("mx"), P("mx"), P("mx", "my"), P("my"), P("mx", "my"), P("my"), P("mx", "my"), P("my"), P("my", "mx"), P("mx", "my"), P("mx", "my"), P("my", "mx"), cache_spec, cache_spec)
    out_specs = (act_spec, cache_spec, cache_spec)

    def local_layer(x_in, seq_lens, gain_attn, gain_mlp, w_q, b_q, w_k, b_k, w_v, b_v, w_o, w_gate, w_up, w_down, k_cache, v_cache):
        hidden = x_in.shape[1] * mx_size
        x_f32 = x_in.astype(jnp.float32)
        attn_sq = lax.psum(jnp.sum(x_f32 * x_f32, axis=1, keepdims=True), "mx")
        normed = (x_f32 * lax.rsqrt(attn_sq / hidden + NORM_EPS) * gain_attn.astype(jnp.float32)).astype(jnp.bfloat16)
        q_cols = w_q.shape[1]
        kv_cols = w_k.shape[1]
        partials = jnp.concatenate([
            jnp.dot(normed, w_q, preferred_element_type=jnp.float32).astype(jnp.bfloat16),
            jnp.dot(normed, w_k, preferred_element_type=jnp.float32).astype(jnp.bfloat16),
            jnp.dot(normed, w_v, preferred_element_type=jnp.float32).astype(jnp.bfloat16),
        ], axis=1)
        projected = lax.psum_scatter(partials, "mx", scatter_dimension=0, tiled=True).astype(jnp.float32)
        q_vals = projected[:, :q_cols] + b_q.astype(jnp.float32)
        k_vals = projected[:, q_cols:q_cols + kv_cols] + b_k.astype(jnp.float32)
        v_vals = projected[:, q_cols + kv_cols:] + b_v.astype(jnp.float32)
        half_dim = HEAD // 2
        inv_freq = ROPE_THETA ** (-2.0 * jnp.arange(half_dim, dtype=jnp.float32) / HEAD)
        angles = seq_lens.astype(jnp.float32)[:, None, None] * inv_freq
        cos_tab, sin_tab = jnp.cos(angles), jnp.sin(angles)
        q_rot = rotate(q_vals, cos_tab, sin_tab)
        k_rot = rotate(k_vals, cos_tab, sin_tab)
        v_new = v_vals.astype(jnp.bfloat16).astype(jnp.float32)
        k_cache_out, v_cache_out, attn_rows = attend(seq_lens, q_rot, k_rot, v_new, k_cache, v_cache)
        attn_all = lax.all_gather(attn_rows, "mx", axis=0, tiled=True)
        attn_proj = lax.psum(jnp.dot(attn_all, w_o, preferred_element_type=jnp.float32).astype(jnp.bfloat16), "my")
        x_mid = (x_f32 + attn_proj.astype(jnp.float32)).astype(jnp.bfloat16)
        mid_f32 = x_mid.astype(jnp.float32)
        mlp_sq = lax.psum(jnp.sum(mid_f32 * mid_f32, axis=1, keepdims=True), "mx")
        normed_mlp = (mid_f32 * lax.rsqrt(mlp_sq / hidden + NORM_EPS) * gain_mlp.astype(jnp.float32)).astype(jnp.bfloat16)
        ff_cols = w_gate.shape[1]
        gate_up = lax.psum(jnp.concatenate([
            jnp.dot(normed_mlp, w_gate, preferred_element_type=jnp.float32).astype(jnp.bfloat16),
            jnp.dot(normed_mlp, w_up, preferred_element_type=jnp.float32).astype(jnp.bfloat16),
        ], axis=1), "mx").astype(jnp.float32)
        hidden_act = (jax.nn.silu(gate_up[:, :ff_cols]) * gate_up[:, ff_cols:]).astype(jnp.bfloat16)
        down_proj = lax.psum(jnp.dot(hidden_act, w_down, preferred_element_type=jnp.float32).astype(jnp.bfloat16), "my")
        x_out = (mid_f32 + down_proj.astype(jnp.float32)).astype(jnp.bfloat16)
        return x_out, k_cache_out, v_cache_out

    return jax.shard_map(local_layer, mesh=mesh, in_specs=in_specs, out_specs=out_specs, check_vma=False)
```

```python
import jax
import jax.numpy as jnp
from jax import lax
from jax.experimental import pallas as pl
from jax.experimental.pallas import tpu as pltpu
from jax.sharding import PartitionSpec as P

HEAD = 128
NORM_EPS = 1e-6
ROPE_THETA = 1000000.0
SLOT_ROWS = 8
SLOTS = 8
AHEAD = 6
PAD_HEADS = 16
CHUNKS = 1
RING = 6
PIECE = 640
TILE = 256
MROWS = 192
ROWS_STEP = 16
MESH = pl.DeviceIdType.MESH


def attend_kernel(lens, q_ref, kn_ref, vn_ref, kc, vc, ko, vo, out_ref, kbuf, vbuf, qs, os, sems):
    rows = q_ref.shape[0]
    heads = q_ref.shape[1] // HEAD
    flat = kbuf.shape[2]
    blocks = rows // SLOT_ROWS

    def moves(block, slot, inward):
        part = pl.ds(block * SLOT_ROWS, SLOT_ROWS)
        if inward:
            return (pltpu.make_async_copy(kc.at[part], kbuf.at[slot], sems.at[0, slot]),
                    pltpu.make_async_copy(vc.at[part], vbuf.at[slot], sems.at[1, slot]))
        return (pltpu.make_async_copy(kbuf.at[slot], ko.at[part], sems.at[2, slot]),
                pltpu.make_async_copy(vbuf.at[slot], vo.at[part], sems.at[3, slot]))

    for block in range(AHEAD):
        for move in moves(block, block, True):
            move.start()
    qs[...] = jnp.zeros_like(qs)

    tile_row = lax.broadcasted_iota(jnp.int32, (PAD_HEADS, HEAD), 0)
    pair_row = lax.broadcasted_iota(jnp.int32, (2 * PAD_HEADS, flat), 0)
    col = lax.broadcasted_iota(jnp.int32, (2 * PAD_HEADS, flat), 1)
    second = pair_row >= PAD_HEADS
    head_of_row = jnp.where(pair_row % PAD_HEADS >= heads // 2, 1, 0)
    col_pos = jnp.where(col % 2 == head_of_row, col // 2, jnp.int32(1 << 20))
    zeros = jnp.zeros((PAD_HEADS, HEAD), jnp.bfloat16)

    def put_row(buf, slot, j, pos, new8):
        base = pl.multiple_of((2 * pos) // 16 * 16, 16)
        off = 2 * pos - base
        tile = buf[slot, j, pl.ds(base, 16), :]
        first = jnp.broadcast_to(new8[j:j + 1, :HEAD], (16, HEAD)).astype(jnp.bfloat16)
        other = jnp.broadcast_to(new8[j:j + 1, HEAD:], (16, HEAD)).astype(jnp.bfloat16)
        tile = jnp.where(tile_row == off, first, jnp.where(tile_row == off + 1, other, tile))
        buf[slot, j, pl.ds(base, 16), :] = tile

    @pl.loop(0, blocks // 2)
    def _(step):
        for half in range(2):
            block = step * 2 + half
            slot = lax.rem(block, SLOTS)
            for move in moves(block, slot, True):
                move.wait()
            rows8 = pl.ds(pl.multiple_of(block * SLOT_ROWS, SLOT_ROWS), SLOT_ROWS)
            kn8, vn8 = kn_ref[rows8, :], vn_ref[rows8, :]
            for h in range(heads):
                qs[pl.ds(h, SLOT_ROWS, stride=PAD_HEADS), :] = q_ref[rows8, h * HEAD:(h + 1) * HEAD]
            for j in range(SLOT_ROWS):
                b = block * SLOT_ROWS + j
                put_row(kbuf, slot, j, lens[b], kn8)
                put_row(vbuf, slot, j, lens[b], vn8)
            pairs = range(0, SLOT_ROWS, 2)
            scores = []
            for j in pairs:
                q0 = qs[j * PAD_HEADS:(j + 1) * PAD_HEADS, :].astype(jnp.bfloat16)
                q1 = qs[(j + 1) * PAD_HEADS:(j + 2) * PAD_HEADS, :].astype(jnp.bfloat16)
                qp = jnp.concatenate([jnp.concatenate([q0, zeros], axis=1), jnp.concatenate([zeros, q1], axis=1)], axis=0)
                kp = jnp.concatenate([kbuf[slot, j], kbuf[slot, j + 1]], axis=1)
                scores.append(lax.dot_general(qp, kp, (((1,), (1,)), ((), ())), preferred_element_type=jnp.float32))
            probs = []
            for i, j in enumerate(pairs):
                b = block * SLOT_ROWS + j
                limit = jnp.where(second, lens[b + 1], lens[b])
                s = jnp.where(col_pos <= limit, scores[i] * HEAD ** -0.5, -jnp.inf)
                e = jnp.exp(s - jnp.max(s, axis=-1, keepdims=True))
                probs.append((e.astype(jnp.bfloat16), jnp.sum(e, axis=-1, keepdims=True)))
            for i, j in enumerate(pairs):
                e, total = probs[i]
                vp = jnp.concatenate([vbuf[slot, j], vbuf[slot, j + 1]], axis=1)
                o = jnp.dot(e, vp, preferred_element_type=jnp.float32)
                at = (half * SLOT_ROWS + j) * PAD_HEADS
                os[at:at + PAD_HEADS, :] = o[:PAD_HEADS, :HEAD] / total[:PAD_HEADS]
                os[at + PAD_HEADS:at + 2 * PAD_HEADS, :] = o[PAD_HEADS:, HEAD:] / total[PAD_HEADS:]
            for move in moves(block, slot, False):
                move.start()

            @pl.when(block + AHEAD < blocks)
            def _():
                later = lax.rem(block + AHEAD, SLOTS)

                @pl.when(block + AHEAD >= SLOTS)
                def _():
                    for move in moves(block + AHEAD - SLOTS, later, False):
                        move.wait()
                for move in moves(block + AHEAD, later, True):
                    move.start()
        for h in range(heads):
            out_ref[pl.ds(pl.multiple_of(step * 16, 16), 16), h * HEAD:(h + 1) * HEAD] = os[pl.ds(h, 16, stride=PAD_HEADS), :].astype(jnp.bfloat16)

    for block in range(blocks - SLOTS, blocks):
        for move in moves(block, block % SLOTS, False):
            move.wait()


def attend(lens, q, k_new, v_new, k_cache, v_cache):
    rows, seq, kv, _ = k_cache.shape
    flat = seq * kv
    kc = k_cache.reshape(rows, flat, HEAD)
    vc = v_cache.reshape(rows, flat, HEAD)
    whole = pl.BlockSpec(memory_space=pltpu.VMEM)
    hbm = pl.BlockSpec(memory_space=pltpu.HBM)
    ko, vo, out = pl.pallas_call(
        attend_kernel,
        out_shape=(jax.ShapeDtypeStruct(kc.shape, kc.dtype), jax.ShapeDtypeStruct(vc.shape, vc.dtype), jax.ShapeDtypeStruct(q.shape, jnp.bfloat16)),
        in_specs=[pl.BlockSpec(memory_space=pltpu.SMEM), whole, whole, whole, hbm, hbm],
        out_specs=(hbm, hbm, whole),
        scratch_shapes=[
            pltpu.VMEM((SLOTS, SLOT_ROWS, flat, HEAD), jnp.bfloat16),
            pltpu.VMEM((SLOTS, SLOT_ROWS, flat, HEAD), jnp.bfloat16),
            pltpu.VMEM((SLOT_ROWS * PAD_HEADS, HEAD), jnp.float32),
            pltpu.VMEM((2 * SLOT_ROWS * PAD_HEADS, HEAD), jnp.float32),
            pltpu.SemaphoreType.DMA((4, SLOTS)),
        ],
        compiler_params=pltpu.CompilerParams(vmem_limit_bytes=40 << 20),
        name="attend",
    )(lens, q, k_new, v_new, kc, vc)
    return ko.reshape(k_cache.shape), vo.reshape(v_cache.shape), out


def tail_kernel(attn_ref, x_hbm, gain_ref, wo_hbm, wg_hbm, wu_hbm, wd_hbm, out_ref,
                attn_all, xown, wo_v, wd_v, ring, sb, rb, keep, mall, hbuf, gsend, grecv, act, ssq, ssr,
                wo_sem, wd_sem, ring_sem, x_sem, ici_ss, ici_rs, gu_ss, gu_rs, act_ss, act_rs, st_ss, st_rs, at_ss, at_rs):
    my, mx = lax.axis_index("my"), lax.axis_index("mx")
    row_count, hidden = out_ref.shape
    half_rows = row_count // 2
    sub = half_rows // CHUNKS
    ff = wg_hbm.shape[1]
    steps = (ff // 128 + 1) // 2 * 128 // TILE
    own_w = steps * TILE
    shift = ff - own_w
    per_chunk = 2 * steps
    total_steps = CHUNKS * per_chunk

    def chunk_of(r):
        return lax.rem(my // 2 + r // 2, 2) * 2 + lax.rem(lax.rem(my, 2) + r % 2, 2)

    def device(r):
        return (chunk_of(r), mx)

    partner = (my, 1 - mx)
    first = lambda s: 1 if s == 0 else 2
    second = lambda s: 2 if s == 0 else 1

    def cols(r):
        return pl.ds(pl.multiple_of(chunk_of(r) * PIECE, 128), PIECE)

    barrier = pltpu.get_barrier_semaphore()
    for peer in (device(1), device(2), partner):
        pl.semaphore_signal(barrier, inc=1, device_id=peer, device_id_type=MESH)

    order = (3, 1, 2, 0)
    wo_copies = {r: pltpu.make_async_copy(wo_hbm.at[:, cols(r)], wo_v.at[r], wo_sem.at[r]) for r in order}
    wd_copies = {r: pltpu.make_async_copy(wd_hbm.at[:, cols(r)], wd_v.at[r], wd_sem.at[r]) for r in order}
    x_copy = pltpu.make_async_copy(x_hbm.at[:, cols(0)], xown, x_sem)
    for r in order:
        wo_copies[r].start()
    x_copy.start()

    def ring_copies(g):
        slot = lax.rem(g, RING)
        at = lax.rem(g, per_chunk)
        mine = at // steps
        side = mine * mx + (1 - mine) * (1 - mx)
        col = pl.multiple_of(side * shift + lax.rem(at, steps) * TILE, 128)
        return (pltpu.make_async_copy(wg_hbm.at[:, pl.ds(col, TILE)], ring.at[slot, :, pl.ds(0, TILE)], ring_sem.at[slot, 0]),
                pltpu.make_async_copy(wu_hbm.at[:, pl.ds(col, TILE)], ring.at[slot, :, pl.ds(TILE, TILE)], ring_sem.at[slot, 1]))

    def remote(src, dst, ss, rs, peer):
        return pltpu.make_async_remote_copy(src_ref=src, dst_ref=dst, send_sem=ss, recv_sem=rs, device_id=peer, device_id_type=MESH)

    def hop(c, s, msg, src, dst, r):
        return remote(src, dst, ici_ss.at[c, s, msg], ici_rs.at[c, s, msg], device(r))

    pl.semaphore_wait(barrier, 3)
    attn_msg = remote(attn_ref, attn_all.at[mx], at_ss, at_rs, partner)
    attn_msg.start()

    def for_rows(count, body):
        @pl.loop(0, count // ROWS_STEP)
        def _(i):
            body(pl.multiple_of(i * ROWS_STEP, ROWS_STEP))

    def copy_attn(at):
        attn_all[mx, pl.ds(at, ROWS_STEP), :] = attn_ref[pl.ds(at, ROWS_STEP), :]
    for_rows(half_rows, copy_attn)

    def rs_msg(c, s, base, k):
        return hop(c, s, base + k, sb.at[c, s, k], rb.at[c, s, k], second(s) if k == 2 else first(s))

    blocks = 2 * sub // MROWS

    def parts(block):
        if CHUNKS == 1:
            return ((block, 0, sub),)
        return ((0, 0, sub), (1, sub, 2 * sub))

    def product(c, r, lhs, weights, base, send):
        for block in range(blocks):
            acc = jnp.dot(lhs(block), weights[...], preferred_element_type=jnp.float32)
            for s, lo, hi in parts(block):
                piece = acc[lo:hi]
                if r == 3 or r == first(s):
                    which = 0 if r == 3 else 1
                    sb[c, s, which] = piece.astype(jnp.bfloat16)
                    if send:
                        rs_msg(c, s, base, which).start()
                else:
                    keep[c, s, 0 if r == second(s) else 1] = piece

    def rs_send(c, base):
        for which in range(2):
            for s in range(2):
                rs_msg(c, s, base, which).start()

    def rs_middle(c, base):
        for s in range(2):
            rs_msg(c, s, base, 0).wait_recv()

            def add(at, s=s):
                rows = pl.ds(at, ROWS_STEP)
                sb[c, s, 2, rows, :] = (keep[c, s, 0, rows, :] + rb[c, s, 0, rows, :].astype(jnp.float32)).astype(jnp.bfloat16)
            for_rows(sub, add)
            rs_msg(c, s, base, 2).start()

    def rs_sum(c, s, rows):
        return keep[c, s, 1, rows, :] + rb[c, s, 1, rows, :].astype(jnp.float32) + rb[c, s, 2, rows, :].astype(jnp.float32)

    def mid_at(c, s, r):
        return mall.at[c, chunk_of(r), pl.ds(s * sub, sub), :]

    def out_at(c, s, r):
        return out_ref.at[pl.ds(s * half_rows + c * sub, sub), cols(r)]

    def ag_msg(c, s, base, at, k):
        src = at(c, s, second(s) if k == 2 else 0)
        return hop(c, s, base + k, src, src, second(s) if k == 0 else first(s))

    def finish_mid(c):
        for s in range(2):
            rs_msg(c, s, 0, 1).wait_recv()
            rs_msg(c, s, 0, 2).wait_recv()

            def add(at, s=s):
                rows = pl.ds(at, ROWS_STEP)
                total = rs_sum(c, s, rows) + xown[pl.ds(s * half_rows + c * sub + at, ROWS_STEP), :].astype(jnp.float32)
                mall[c, my, pl.ds(s * sub + at, ROWS_STEP), :] = total.astype(jnp.bfloat16)
            for_rows(sub, add)
            ag_msg(c, s, 3, mid_at, 0).start()
            ag_msg(c, s, 3, mid_at, 1).start()

    def finish_out(c):
        for s in range(2):
            rs_msg(c, s, 6, 1).wait_recv()
            rs_msg(c, s, 6, 2).wait_recv()

            def add(at, s=s):
                rows = pl.ds(at, ROWS_STEP)
                total = rs_sum(c, s, rows) + mall[c, my, pl.ds(s * sub + at, ROWS_STEP), :].astype(jnp.float32)
                out_ref[pl.ds(s * half_rows + c * sub + at, ROWS_STEP), cols(0)] = total.astype(jnp.bfloat16)
            for_rows(sub, add)
            ag_msg(c, s, 9, out_at, 0).start()
            ag_msg(c, s, 9, out_at, 1).start()

    def forward(c, base, at):
        for s in range(2):
            ag_msg(c, s, base, at, 0).wait_recv()
            ag_msg(c, s, base, at, 2).start()

    def arrive(c, base, at):
        for s in range(2):
            ag_msg(c, s, base, at, 1).wait_recv()
            ag_msg(c, s, base, at, 2).wait_recv()

    def sent(c, base, at=None):
        for s in range(2):
            for k in range(3):
                (rs_msg(c, s, base, k) if at is None else ag_msg(c, s, base, at, k)).wait_send()

    def normalise(c):
        def squares(at):
            rows = pl.ds(at, ROWS_STEP)
            total = jnp.zeros((ROWS_STEP, 128), jnp.float32)
            for j in range(4):
                for k in range(0, PIECE, 128):
                    m = mall[c, j, rows, k:k + 128].astype(jnp.float32)
                    total = total + m * m
            ssq[c, rows, :] = total
        for_rows(2 * sub, squares)
        msg = remote(ssq.at[c], ssr.at[c], st_ss.at[c], st_rs.at[c], partner)
        msg.start()
        msg.wait()

        def scale(at):
            rows = pl.ds(at, ROWS_STEP)
            total = jnp.sum(ssq[c, rows, :] + ssr[c, rows, :], axis=1, keepdims=True)
            inv = lax.rsqrt(total / (2 * hidden) + NORM_EPS)
            for j in range(4):
                at_col = slice(j * PIECE, (j + 1) * PIECE)
                hbuf[rows, at_col] = (mall[c, j, rows, :].astype(jnp.float32) * inv * gain_ref[:, at_col]).astype(jnp.bfloat16)
        for_rows(2 * sub, scale)

    def gu_msg(c, t):
        return remote(gsend.at[t], grecv.at[t], gu_ss.at[c, t], gu_rs.at[c, t], partner)

    def tiles(c, mine, lo, hi):
        @pl.loop(lo, hi)
        def _(t):
            g = c * per_chunk + mine * steps + t
            slot = lax.rem(g, RING)
            for copy in ring_copies(g):
                copy.wait()
            if mine:
                gu_msg(c, t).wait_recv()
            for block in range(blocks):
                rows = slice(block * MROWS, (block + 1) * MROWS)
                acc = jnp.dot(hbuf[rows, :], ring[slot], preferred_element_type=jnp.float32)
                if mine:
                    both = acc + grecv[t, rows, :].astype(jnp.float32)
                    gate, up = both[:, :TILE], both[:, TILE:]
                    act[rows, pl.ds(pl.multiple_of(mx * shift + t * TILE, 128), TILE)] = (gate * jax.nn.sigmoid(gate) * up).astype(jnp.bfloat16)
                else:
                    gsend[t, rows, :] = acc.astype(jnp.bfloat16)
            if not mine:
                gu_msg(c, t).start()

            @pl.when(g + RING < total_steps)
            def _():
                for copy in ring_copies(g + RING):
                    copy.start()

    cut = 3 * TILE

    def act_msg(c, k):
        width = cut if k == 0 else shift - cut
        where = pl.ds(pl.multiple_of(mx * own_w + (0 if k == 0 else cut), 128), width)
        return remote(act.at[:, where], act.at[:, where], act_ss.at[c, k], act_rs.at[c, k], partner)

    def gates_sent(c):
        for t in range(steps):
            gu_msg(c, t).wait_send()

    def attn_lhs(c):
        def get(block):
            if CHUNKS == 1:
                return attn_all[block]
            rows = slice(c * sub, (c + 1) * sub)
            return jnp.concatenate([attn_all[0, rows, :], attn_all[1, rows, :]], axis=0)
        return get

    def act_lhs(block):
        return act[block * MROWS:(block + 1) * MROWS, :]

    attn_msg.wait_recv()
    for r in order:
        wo_copies[r].wait()
        if r == 3:
            for g in range(RING):
                for copy in ring_copies(g):
                    copy.start()
        product(0, r, attn_lhs(0), wo_v.at[r], 0, True)
    x_copy.wait()
    for r in order:
        wd_copies[r].start()
    rs_middle(0, 0)
    finish_mid(0)
    forward(0, 3, mid_at)
    arrive(0, 3, mid_at)
    normalise(0)
    tiles(0, 0, 0, steps)
    tiles(0, 1, 0, 4)
    act_msg(0, 0).start()
    tiles(0, 1, 4, steps)
    act_msg(0, 1).start()
    sent(0, 0)
    for k in range(2):
        act_msg(0, k).wait_recv()
    for r in order:
        wd_copies[r].wait()
        product(0, r, act_lhs, wd_v.at[r], 6, True)
    rs_middle(0, 6)
    finish_out(0)
    forward(0, 9, out_at)
    arrive(0, 9, out_at)
    gates_sent(0)
    for k in range(2):
        act_msg(0, k).wait_send()
    sent(0, 3, mid_at)
    sent(0, 6)
    sent(0, 9, out_at)
    attn_msg.wait_send()


def tail(attn, x_in, gain, w_o, w_gate, w_up, w_down):
    rows, hidden = x_in.shape
    q_width = w_o.shape[0]
    ff = w_gate.shape[1]
    sub = rows // 2 // CHUNKS
    steps = (ff // 128 + 1) // 2 * 128 // TILE
    whole = pl.BlockSpec(memory_space=pltpu.VMEM)
    hbm = pl.BlockSpec(memory_space=pltpu.HBM)
    bf16, f32 = jnp.bfloat16, jnp.float32
    dma = pltpu.SemaphoreType.DMA
    return pl.pallas_call(
        tail_kernel,
        out_shape=jax.ShapeDtypeStruct((rows, hidden), bf16),
        in_specs=[whole, hbm, whole, hbm, hbm, hbm, hbm],
        out_specs=whole,
        scratch_shapes=[
            pltpu.VMEM((2, rows // 2, q_width), bf16),
            pltpu.VMEM((rows, PIECE), bf16),
            pltpu.VMEM((4, q_width, PIECE), bf16),
            pltpu.VMEM((4, ff, PIECE), bf16),
            pltpu.VMEM((RING, hidden, 2 * TILE), bf16),
            pltpu.VMEM((CHUNKS, 2, 3, sub, PIECE), bf16),
            pltpu.VMEM((CHUNKS, 2, 3, sub, PIECE), bf16),
            pltpu.VMEM((CHUNKS, 2, 2, sub, PIECE), f32),
            pltpu.VMEM((CHUNKS, 4, 2 * sub, PIECE), bf16),
            pltpu.VMEM((2 * sub, hidden), bf16),
            pltpu.VMEM((steps, 2 * sub, 2 * TILE), bf16),
            pltpu.VMEM((steps, 2 * sub, 2 * TILE), bf16),
            pltpu.VMEM((2 * sub, ff), bf16),
            pltpu.VMEM((CHUNKS, 2 * sub, 128), f32),
            pltpu.VMEM((CHUNKS, 2 * sub, 128), f32),
            dma((4,)), dma((4,)), dma((RING, 2)), dma(()),
            dma((CHUNKS, 2, 12)), dma((CHUNKS, 2, 12)),
            dma((CHUNKS, steps)), dma((CHUNKS, steps)),
            dma((CHUNKS, 2)), dma((CHUNKS, 2)),
            dma((CHUNKS,)), dma((CHUNKS,)),
            dma(()), dma(()),
        ],
        compiler_params=pltpu.CompilerParams(collective_id=1, has_side_effects=True, vmem_limit_bytes=67043328),
        name="tail",
    )(attn, x_in, gain, w_o, w_gate, w_up, w_down)


def rotate(cols, cos_tab, sin_tab):
    rows, width = cols.shape
    heads = cols.reshape(rows, width // HEAD, HEAD)
    lower, upper = heads[..., :HEAD // 2], heads[..., HEAD // 2:]
    out = jnp.concatenate([lower * cos_tab - upper * sin_tab, upper * cos_tab + lower * sin_tab], axis=-1)
    return out.astype(jnp.bfloat16).astype(jnp.float32).reshape(rows, width)


def solution(mesh):
    mx_size = mesh.shape["mx"]
    act_spec = P(None, "mx")
    cache_spec = P("mx", None, "my", None)
    in_specs = (act_spec, P("mx"), P("mx"), P("mx"), P("mx", "my"), P("my"), P("mx", "my"), P("my"), P("mx", "my"), P("my"), P("my", "mx"), P("mx", "my"), P("mx", "my"), P("my", "mx"), cache_spec, cache_spec)
    out_specs = (act_spec, cache_spec, cache_spec)

    def local_layer(x_in, seq_lens, gain_attn, gain_mlp, w_q, b_q, w_k, b_k, w_v, b_v, w_o, w_gate, w_up, w_down, k_cache, v_cache):
        hidden = x_in.shape[1] * mx_size
        x_f32 = x_in.astype(jnp.float32)
        attn_sq = lax.psum(jnp.sum(x_f32 * x_f32, axis=1, keepdims=True), "mx")
        normed = (x_f32 * lax.rsqrt(attn_sq / hidden + NORM_EPS) * gain_attn.astype(jnp.float32)).astype(jnp.bfloat16)
        q_cols = w_q.shape[1]
        kv_cols = w_k.shape[1]
        partials = jnp.concatenate([
            jnp.dot(normed, w_q, preferred_element_type=jnp.float32).astype(jnp.bfloat16),
            jnp.dot(normed, w_k, preferred_element_type=jnp.float32).astype(jnp.bfloat16),
            jnp.dot(normed, w_v, preferred_element_type=jnp.float32).astype(jnp.bfloat16),
        ], axis=1)
        projected = lax.psum_scatter(partials, "mx", scatter_dimension=0, tiled=True).astype(jnp.float32)
        q_vals = projected[:, :q_cols] + b_q.astype(jnp.float32)
        k_vals = projected[:, q_cols:q_cols + kv_cols] + b_k.astype(jnp.float32)
        v_vals = projected[:, q_cols + kv_cols:] + b_v.astype(jnp.float32)
        half_dim = HEAD // 2
        inv_freq = ROPE_THETA ** (-2.0 * jnp.arange(half_dim, dtype=jnp.float32) / HEAD)
        angles = seq_lens.astype(jnp.float32)[:, None, None] * inv_freq
        cos_tab, sin_tab = jnp.cos(angles), jnp.sin(angles)
        q_rot = rotate(q_vals, cos_tab, sin_tab)
        k_rot = rotate(k_vals, cos_tab, sin_tab)
        v_new = v_vals.astype(jnp.bfloat16).astype(jnp.float32)
        k_cache_out, v_cache_out, attn_rows = attend(seq_lens, q_rot, k_rot, v_new, k_cache, v_cache)
        x_out = tail(attn_rows, x_in, gain_mlp.astype(jnp.float32)[None, :], w_o, w_gate, w_up, w_down)
        return x_out, k_cache_out, v_cache_out

    return jax.shard_map(local_layer, mesh=mesh, in_specs=in_specs, out_specs=out_specs, check_vma=False)
```

```python
import jax
import jax.numpy as jnp
import numpy as np
from jax import lax
from jax.experimental import pallas as pl
from jax.experimental.pallas import tpu as pltpu
from jax.sharding import PartitionSpec as P

HEAD = 128
NORM_EPS = 1e-6
ROPE_THETA = 1000000.0
SLOT_ROWS = 8
SLOTS = 8
AHEAD = 6
PAD_HEADS = 16
CHUNKS = 1
RING = 6
PIECE = 640
TILE = 256
MROWS = 192
ROWS_STEP = 16
MESH = pl.DeviceIdType.MESH


def attend_kernel(lens, q_hbm, kn_hbm, vn_hbm, kc, vc, ko, vo, out_hbm, kbuf, vbuf, q_ref, kn_ref, vn_ref, out_ref, qs, os, sems, in_sem, out_sem):
    rows = q_ref.shape[0]
    heads = q_ref.shape[1] // HEAD
    flat = kbuf.shape[2]
    blocks = rows // SLOT_ROWS

    def moves(block, slot, inward):
        part = pl.ds(block * SLOT_ROWS, SLOT_ROWS)
        if inward:
            return (pltpu.make_async_copy(kc.at[part], kbuf.at[slot], sems.at[0, slot]),
                    pltpu.make_async_copy(vc.at[part], vbuf.at[slot], sems.at[1, slot]))
        return (pltpu.make_async_copy(kbuf.at[slot], ko.at[part], sems.at[2, slot]),
                pltpu.make_async_copy(vbuf.at[slot], vo.at[part], sems.at[3, slot]))

    for block in range(AHEAD):
        for move in moves(block, block, True):
            move.start()
    loads = [pltpu.make_async_copy(src, dst, in_sem.at[i]) for i, (src, dst) in enumerate(((q_hbm, q_ref), (kn_hbm, kn_ref), (vn_hbm, vn_ref)))]
    for load in loads:
        load.start()
    qs[...] = jnp.zeros_like(qs)

    def put_out(step):
        part = pl.ds(pl.multiple_of(step * 16, 16), 16)
        return pltpu.make_async_copy(out_ref.at[part], out_hbm.at[part], out_sem)

    tile_row = lax.broadcasted_iota(jnp.int32, (PAD_HEADS, HEAD), 0)
    pair_row = lax.broadcasted_iota(jnp.int32, (2 * PAD_HEADS, flat), 0)
    col = lax.broadcasted_iota(jnp.int32, (2 * PAD_HEADS, flat), 1)
    second = pair_row >= PAD_HEADS
    head_of_row = jnp.where(pair_row % PAD_HEADS >= heads // 2, 1, 0)
    col_pos = jnp.where(col % 2 == head_of_row, col // 2, jnp.int32(1 << 20))
    zeros = jnp.zeros((PAD_HEADS, HEAD), jnp.bfloat16)

    def put_row(buf, slot, j, pos, new8):
        base = pl.multiple_of((2 * pos) // 16 * 16, 16)
        off = 2 * pos - base
        tile = buf[slot, j, pl.ds(base, 16), :]
        first = jnp.broadcast_to(new8[j:j + 1, :HEAD], (16, HEAD)).astype(jnp.bfloat16)
        other = jnp.broadcast_to(new8[j:j + 1, HEAD:], (16, HEAD)).astype(jnp.bfloat16)
        tile = jnp.where(tile_row == off, first, jnp.where(tile_row == off + 1, other, tile))
        buf[slot, j, pl.ds(base, 16), :] = tile

    for load in loads:
        load.wait()

    @pl.loop(0, blocks // 2)
    def _(step):
        for half in range(2):
            block = step * 2 + half
            slot = lax.rem(block, SLOTS)
            for move in moves(block, slot, True):
                move.wait()
            rows8 = pl.ds(pl.multiple_of(block * SLOT_ROWS, SLOT_ROWS), SLOT_ROWS)
            kn8, vn8 = kn_ref[rows8, :], vn_ref[rows8, :]
            for h in range(heads):
                qs[pl.ds(h, SLOT_ROWS, stride=PAD_HEADS), :] = q_ref[rows8, h * HEAD:(h + 1) * HEAD]
            for j in range(SLOT_ROWS):
                b = block * SLOT_ROWS + j
                put_row(kbuf, slot, j, lens[b], kn8)
                put_row(vbuf, slot, j, lens[b], vn8)
            pairs = range(0, SLOT_ROWS, 2)
            scores = []
            for j in pairs:
                q0 = qs[j * PAD_HEADS:(j + 1) * PAD_HEADS, :].astype(jnp.bfloat16)
                q1 = qs[(j + 1) * PAD_HEADS:(j + 2) * PAD_HEADS, :].astype(jnp.bfloat16)
                qp = jnp.concatenate([jnp.concatenate([q0, zeros], axis=1), jnp.concatenate([zeros, q1], axis=1)], axis=0)
                kp = jnp.concatenate([kbuf[slot, j], kbuf[slot, j + 1]], axis=1)
                scores.append(lax.dot_general(qp, kp, (((1,), (1,)), ((), ())), preferred_element_type=jnp.float32))
            probs = []
            for i, j in enumerate(pairs):
                b = block * SLOT_ROWS + j
                limit = jnp.where(second, lens[b + 1], lens[b])
                s = jnp.where(col_pos <= limit, scores[i] * HEAD ** -0.5, -jnp.inf)
                e = jnp.exp(s - jnp.max(s, axis=-1, keepdims=True))
                probs.append((e.astype(jnp.bfloat16), jnp.sum(e, axis=-1, keepdims=True)))
            for i, j in enumerate(pairs):
                e, total = probs[i]
                vp = jnp.concatenate([vbuf[slot, j], vbuf[slot, j + 1]], axis=1)
                o = jnp.dot(e, vp, preferred_element_type=jnp.float32)
                at = (half * SLOT_ROWS + j) * PAD_HEADS
                os[at:at + PAD_HEADS, :] = o[:PAD_HEADS, :HEAD] / total[:PAD_HEADS]
                os[at + PAD_HEADS:at + 2 * PAD_HEADS, :] = o[PAD_HEADS:, HEAD:] / total[PAD_HEADS:]
            for move in moves(block, slot, False):
                move.start()

            @pl.when(block + AHEAD < blocks)
            def _():
                later = lax.rem(block + AHEAD, SLOTS)

                @pl.when(block + AHEAD >= SLOTS)
                def _():
                    for move in moves(block + AHEAD - SLOTS, later, False):
                        move.wait()
                for move in moves(block + AHEAD, later, True):
                    move.start()
        for h in range(heads):
            out_ref[pl.ds(pl.multiple_of(step * 16, 16), 16), h * HEAD:(h + 1) * HEAD] = os[pl.ds(h, 16, stride=PAD_HEADS), :].astype(jnp.bfloat16)

        @pl.when(step > 0)
        def _():
            put_out(step - 1).wait()
        put_out(step).start()

    put_out(blocks // 2 - 1).wait()
    for block in range(blocks - SLOTS, blocks):
        for move in moves(block, block % SLOTS, False):
            move.wait()


def attend(lens, q, k_new, v_new, k_cache, v_cache):
    rows, seq, kv, _ = k_cache.shape
    flat = seq * kv
    kc = k_cache.reshape(rows, flat, HEAD)
    vc = v_cache.reshape(rows, flat, HEAD)
    hbm = pl.BlockSpec(memory_space=pltpu.HBM)
    ko, vo, out = pl.pallas_call(
        attend_kernel,
        out_shape=(jax.ShapeDtypeStruct(kc.shape, kc.dtype), jax.ShapeDtypeStruct(vc.shape, vc.dtype), jax.ShapeDtypeStruct(q.shape, jnp.bfloat16)),
        in_specs=[pl.BlockSpec(memory_space=pltpu.SMEM)] + [hbm] * 5,
        out_specs=(hbm, hbm, hbm),
        scratch_shapes=[
            pltpu.VMEM((SLOTS, SLOT_ROWS, flat, HEAD), jnp.bfloat16),
            pltpu.VMEM((SLOTS, SLOT_ROWS, flat, HEAD), jnp.bfloat16),
            pltpu.VMEM(q.shape, q.dtype),
            pltpu.VMEM(k_new.shape, k_new.dtype),
            pltpu.VMEM(v_new.shape, v_new.dtype),
            pltpu.VMEM(q.shape, jnp.bfloat16),
            pltpu.VMEM((SLOT_ROWS * PAD_HEADS, HEAD), jnp.float32),
            pltpu.VMEM((2 * SLOT_ROWS * PAD_HEADS, HEAD), jnp.float32),
            pltpu.SemaphoreType.DMA((4, SLOTS)),
            pltpu.SemaphoreType.DMA((3,)),
            pltpu.SemaphoreType.DMA(()),
        ],
        compiler_params=pltpu.CompilerParams(vmem_limit_bytes=67043328),
        name="attend",
    )(lens, q, k_new, v_new, kc, vc)
    return ko.reshape(k_cache.shape), vo.reshape(v_cache.shape), out


def tail_kernel(attn_hbm, x_hbm, gain_ref, wo_hbm, wg_hbm, wu_hbm, wd_hbm, out_ref,
                attn_all, xown, wo_v, wd_v, ring, sb, rb, keep, mall, hbuf, gsend, grecv, act, ssq, ssr,
                wo_sem, wd_sem, ring_sem, x_sem, ici_ss, ici_rs, gu_ss, gu_rs, act_ss, act_rs, st_ss, st_rs, at_ss, at_rs, at_sem):
    my, mx = lax.axis_index("my"), lax.axis_index("mx")
    row_count, hidden = out_ref.shape
    half_rows = row_count // 2
    sub = half_rows // CHUNKS
    ff = wg_hbm.shape[1]
    steps = (ff // 128 + 1) // 2 * 128 // TILE
    own_w = steps * TILE
    shift = ff - own_w
    per_chunk = 2 * steps
    total_steps = CHUNKS * per_chunk

    def chunk_of(r):
        return lax.rem(my // 2 + r // 2, 2) * 2 + lax.rem(lax.rem(my, 2) + r % 2, 2)

    def device(r):
        return (chunk_of(r), mx)

    partner = (my, 1 - mx)
    first = lambda s: 1 if s == 0 else 2
    second = lambda s: 2 if s == 0 else 1

    def cols(r):
        return pl.ds(pl.multiple_of(chunk_of(r) * PIECE, 128), PIECE)

    barrier = pltpu.get_barrier_semaphore()
    for peer in (device(1), device(2), partner):
        pl.semaphore_signal(barrier, inc=1, device_id=peer, device_id_type=MESH)

    attn_copy = pltpu.make_async_copy(attn_hbm, attn_all.at[mx], at_sem)
    attn_copy.start()
    order = (3, 1, 2, 0)
    wo_copies = {r: pltpu.make_async_copy(wo_hbm.at[:, cols(r)], wo_v.at[r], wo_sem.at[r]) for r in order}
    wd_copies = {r: pltpu.make_async_copy(wd_hbm.at[:, cols(r)], wd_v.at[r], wd_sem.at[r]) for r in order}
    x_copy = pltpu.make_async_copy(x_hbm.at[:, cols(0)], xown, x_sem)
    for r in order:
        wo_copies[r].start()
    x_copy.start()

    def ring_copies(g):
        slot = lax.rem(g, RING)
        at = lax.rem(g, per_chunk)
        mine = at // steps
        side = mine * mx + (1 - mine) * (1 - mx)
        col = pl.multiple_of(side * shift + lax.rem(at, steps) * TILE, 128)
        return (pltpu.make_async_copy(wg_hbm.at[:, pl.ds(col, TILE)], ring.at[slot, :, pl.ds(0, TILE)], ring_sem.at[slot, 0]),
                pltpu.make_async_copy(wu_hbm.at[:, pl.ds(col, TILE)], ring.at[slot, :, pl.ds(TILE, TILE)], ring_sem.at[slot, 1]))

    def remote(src, dst, ss, rs, peer):
        return pltpu.make_async_remote_copy(src_ref=src, dst_ref=dst, send_sem=ss, recv_sem=rs, device_id=peer, device_id_type=MESH)

    def hop(c, s, msg, src, dst, r):
        return remote(src, dst, ici_ss.at[c, s, msg], ici_rs.at[c, s, msg], device(r))

    attn_copy.wait()
    pl.semaphore_wait(barrier, 3)
    attn_msg = remote(attn_all.at[mx], attn_all.at[mx], at_ss, at_rs, partner)
    attn_msg.start()

    def for_rows(count, body):
        @pl.loop(0, count // ROWS_STEP)
        def _(i):
            body(pl.multiple_of(i * ROWS_STEP, ROWS_STEP))

    def rs_msg(c, s, base, k):
        return hop(c, s, base + k, sb.at[c, s, k], rb.at[c, s, k], second(s) if k == 2 else first(s))

    blocks = 2 * sub // MROWS

    def parts(block):
        if CHUNKS == 1:
            return ((block, 0, sub),)
        return ((0, 0, sub), (1, sub, 2 * sub))

    def product(c, r, lhs, weights, base, send):
        for block in range(blocks):
            acc = jnp.dot(lhs(block), weights[...], preferred_element_type=jnp.float32)
            for s, lo, hi in parts(block):
                piece = acc[lo:hi]
                if r == 3 or r == first(s):
                    which = 0 if r == 3 else 1
                    sb[c, s, which] = piece.astype(jnp.bfloat16)
                    if send:
                        rs_msg(c, s, base, which).start()
                else:
                    keep[c, s, 0 if r == second(s) else 1] = piece

    def rs_send(c, base):
        for which in range(2):
            for s in range(2):
                rs_msg(c, s, base, which).start()

    def rs_middle(c, base):
        for s in range(2):
            rs_msg(c, s, base, 0).wait_recv()

            def add(at, s=s):
                rows = pl.ds(at, ROWS_STEP)
                sb[c, s, 2, rows, :] = (keep[c, s, 0, rows, :] + rb[c, s, 0, rows, :].astype(jnp.float32)).astype(jnp.bfloat16)
            for_rows(sub, add)
            rs_msg(c, s, base, 2).start()

    def rs_sum(c, s, rows):
        return keep[c, s, 1, rows, :] + rb[c, s, 1, rows, :].astype(jnp.float32) + rb[c, s, 2, rows, :].astype(jnp.float32)

    def mid_at(c, s, r):
        return mall.at[c, chunk_of(r), pl.ds(s * sub, sub), :]

    def out_at(c, s, r):
        return out_ref.at[pl.ds(s * half_rows + c * sub, sub), cols(r)]

    def ag_msg(c, s, base, at, k):
        src = at(c, s, second(s) if k == 2 else 0)
        return hop(c, s, base + k, src, src, second(s) if k == 0 else first(s))

    def finish_mid(c):
        for s in range(2):
            rs_msg(c, s, 0, 1).wait_recv()
            rs_msg(c, s, 0, 2).wait_recv()

            def add(at, s=s):
                rows = pl.ds(at, ROWS_STEP)
                total = rs_sum(c, s, rows) + xown[pl.ds(s * half_rows + c * sub + at, ROWS_STEP), :].astype(jnp.float32)
                mall[c, my, pl.ds(s * sub + at, ROWS_STEP), :] = total.astype(jnp.bfloat16)
            for_rows(sub, add)
            ag_msg(c, s, 3, mid_at, 0).start()
            ag_msg(c, s, 3, mid_at, 1).start()

    def finish_out(c):
        for s in range(2):
            rs_msg(c, s, 6, 1).wait_recv()
            rs_msg(c, s, 6, 2).wait_recv()

            def add(at, s=s):
                rows = pl.ds(at, ROWS_STEP)
                total = rs_sum(c, s, rows) + mall[c, my, pl.ds(s * sub + at, ROWS_STEP), :].astype(jnp.float32)
                out_ref[pl.ds(s * half_rows + c * sub + at, ROWS_STEP), cols(0)] = total.astype(jnp.bfloat16)
            for_rows(sub, add)
            ag_msg(c, s, 9, out_at, 0).start()
            ag_msg(c, s, 9, out_at, 1).start()

    def forward(c, base, at):
        for s in range(2):
            ag_msg(c, s, base, at, 0).wait_recv()
            ag_msg(c, s, base, at, 2).start()

    def arrive(c, base, at):
        for s in range(2):
            ag_msg(c, s, base, at, 1).wait_recv()
            ag_msg(c, s, base, at, 2).wait_recv()

    def sent(c, base, at=None):
        for s in range(2):
            for k in range(3):
                (rs_msg(c, s, base, k) if at is None else ag_msg(c, s, base, at, k)).wait_send()

    def normalise(c):
        def squares(at):
            rows = pl.ds(at, ROWS_STEP)
            total = jnp.zeros((ROWS_STEP, 128), jnp.float32)
            for j in range(4):
                for k in range(0, PIECE, 128):
                    m = mall[c, j, rows, k:k + 128].astype(jnp.float32)
                    total = total + m * m
            ssq[c, rows, :] = total
        for_rows(2 * sub, squares)
        msg = remote(ssq.at[c], ssr.at[c], st_ss.at[c], st_rs.at[c], partner)
        msg.start()
        msg.wait()

        def scale(at):
            rows = pl.ds(at, ROWS_STEP)
            total = jnp.sum(ssq[c, rows, :] + ssr[c, rows, :], axis=1, keepdims=True)
            inv = lax.rsqrt(total / (2 * hidden) + NORM_EPS)
            for j in range(4):
                for k in range(PIECE // 128):
                    tile = j * (PIECE // 128) + k
                    m = mall[c, j, rows, k * 128:(k + 1) * 128].astype(jnp.float32)
                    hbuf[rows, tile * 128:(tile + 1) * 128] = (m * inv * gain_ref[tile:tile + 1, :].astype(jnp.float32)).astype(jnp.bfloat16)
        for_rows(2 * sub, scale)

    def gu_msg(c, t):
        return remote(gsend.at[t], grecv.at[t], gu_ss.at[c, t], gu_rs.at[c, t], partner)

    def tiles(c, mine, lo, hi):
        @pl.loop(lo, hi)
        def _(t):
            g = c * per_chunk + mine * steps + t
            slot = lax.rem(g, RING)
            for copy in ring_copies(g):
                copy.wait()
            if mine:
                gu_msg(c, t).wait_recv()
            for block in range(blocks):
                rows = slice(block * MROWS, (block + 1) * MROWS)
                acc = jnp.dot(hbuf[rows, :], ring[slot], preferred_element_type=jnp.float32)
                if mine:
                    both = acc + grecv[t, rows, :].astype(jnp.float32)
                    gate, up = both[:, :TILE], both[:, TILE:]
                    act[rows, pl.ds(pl.multiple_of(mx * shift + t * TILE, 128), TILE)] = (gate * jax.nn.sigmoid(gate) * up).astype(jnp.bfloat16)
                else:
                    gsend[t, rows, :] = acc.astype(jnp.bfloat16)
            if not mine:
                gu_msg(c, t).start()

            @pl.when(g + RING < total_steps)
            def _():
                for copy in ring_copies(g + RING):
                    copy.start()

    cut = 3 * TILE

    def act_msg(c, k):
        width = cut if k == 0 else shift - cut
        where = pl.ds(pl.multiple_of(mx * own_w + (0 if k == 0 else cut), 128), width)
        return remote(act.at[:, where], act.at[:, where], act_ss.at[c, k], act_rs.at[c, k], partner)

    def gates_sent(c):
        for t in range(steps):
            gu_msg(c, t).wait_send()

    def attn_lhs(c):
        def get(block):
            if CHUNKS == 1:
                return attn_all[block]
            rows = slice(c * sub, (c + 1) * sub)
            return jnp.concatenate([attn_all[0, rows, :], attn_all[1, rows, :]], axis=0)
        return get

    def act_lhs(block):
        return act[block * MROWS:(block + 1) * MROWS, :]

    attn_msg.wait_recv()
    for r in order:
        wo_copies[r].wait()
        if r == 3:
            for g in range(RING):
                for copy in ring_copies(g):
                    copy.start()
        product(0, r, attn_lhs(0), wo_v.at[r], 0, True)
    x_copy.wait()
    for r in order:
        wd_copies[r].start()
    rs_middle(0, 0)
    finish_mid(0)
    forward(0, 3, mid_at)
    arrive(0, 3, mid_at)
    normalise(0)
    tiles(0, 0, 0, steps)
    tiles(0, 1, 0, 4)
    act_msg(0, 0).start()
    tiles(0, 1, 4, steps)
    act_msg(0, 1).start()
    sent(0, 0)
    for k in range(2):
        act_msg(0, k).wait_recv()
    for r in order:
        wd_copies[r].wait()
        product(0, r, act_lhs, wd_v.at[r], 6, True)
    rs_middle(0, 6)
    finish_out(0)
    forward(0, 9, out_at)
    arrive(0, 9, out_at)
    gates_sent(0)
    for k in range(2):
        act_msg(0, k).wait_send()
    sent(0, 3, mid_at)
    sent(0, 6)
    sent(0, 9, out_at)
    attn_msg.wait_send()


def tail(attn, x_in, gain, w_o, w_gate, w_up, w_down):
    rows, hidden = x_in.shape
    q_width = w_o.shape[0]
    ff = w_gate.shape[1]
    sub = rows // 2 // CHUNKS
    steps = (ff // 128 + 1) // 2 * 128 // TILE
    whole = pl.BlockSpec(memory_space=pltpu.VMEM)
    hbm = pl.BlockSpec(memory_space=pltpu.HBM)
    bf16, f32 = jnp.bfloat16, jnp.float32
    dma = pltpu.SemaphoreType.DMA
    return pl.pallas_call(
        tail_kernel,
        out_shape=jax.ShapeDtypeStruct((rows, hidden), bf16),
        in_specs=[hbm, hbm, whole, hbm, hbm, hbm, hbm],
        out_specs=whole,
        scratch_shapes=[
            pltpu.VMEM((2, rows // 2, q_width), bf16),
            pltpu.VMEM((rows, PIECE), bf16),
            pltpu.VMEM((4, q_width, PIECE), bf16),
            pltpu.VMEM((4, ff, PIECE), bf16),
            pltpu.VMEM((RING, hidden, 2 * TILE), bf16),
            pltpu.VMEM((CHUNKS, 2, 3, sub, PIECE), bf16),
            pltpu.VMEM((CHUNKS, 2, 3, sub, PIECE), bf16),
            pltpu.VMEM((CHUNKS, 2, 2, sub, PIECE), f32),
            pltpu.VMEM((CHUNKS, 4, 2 * sub, PIECE), bf16),
            pltpu.VMEM((2 * sub, hidden), bf16),
            pltpu.VMEM((steps, 2 * sub, 2 * TILE), bf16),
            pltpu.VMEM((steps, 2 * sub, 2 * TILE), bf16),
            pltpu.VMEM((2 * sub, ff), bf16),
            pltpu.VMEM((CHUNKS, 2 * sub, 128), f32),
            pltpu.VMEM((CHUNKS, 2 * sub, 128), f32),
            dma((4,)), dma((4,)), dma((RING, 2)), dma(()),
            dma((CHUNKS, 2, 12)), dma((CHUNKS, 2, 12)),
            dma((CHUNKS, steps)), dma((CHUNKS, steps)),
            dma((CHUNKS, 2)), dma((CHUNKS, 2)),
            dma((CHUNKS,)), dma((CHUNKS,)),
            dma(()), dma(()), dma(()),
        ],
        compiler_params=pltpu.CompilerParams(collective_id=1, has_side_effects=True, vmem_limit_bytes=67043328),
        name="tail",
    )(attn, x_in, gain, w_o, w_gate, w_up, w_down)


def head_kernel(x_hbm, gain_ref, bq_ref, bk_ref, bv_ref, cos_ref, sin_ref, wq_hbm, wk_hbm, wv_hbm, q_out, k_out, v_out,
                xv, wv_all, hbuf, keep, psend, precv, ssq, ssr, x_sem, w_sem, st_ss, st_rs, p_ss, p_rs):
    my, mx = lax.axis_index("my"), lax.axis_index("mx")
    rows, hidden = xv.shape
    half = rows // 2
    q_cols, kv_cols = wq_hbm.shape[1], wk_hbm.shape[1]
    width = q_cols + 2 * kv_cols
    partner = (my, 1 - mx)
    barrier = pltpu.get_barrier_semaphore()
    pl.semaphore_signal(barrier, inc=1, device_id=partner, device_id_type=MESH)

    x_parts = 4
    x_rows = rows // x_parts
    x_copies = [pltpu.make_async_copy(x_hbm.at[pl.ds(i * x_rows, x_rows)], xv.at[pl.ds(i * x_rows, x_rows)], x_sem.at[i]) for i in range(x_parts)]
    w_copies = [
        pltpu.make_async_copy(wq_hbm, wv_all.at[:, pl.ds(0, q_cols)], w_sem.at[0]),
        pltpu.make_async_copy(wk_hbm, wv_all.at[:, pl.ds(q_cols, kv_cols)], w_sem.at[1]),
        pltpu.make_async_copy(wv_hbm, wv_all.at[:, pl.ds(q_cols + kv_cols, kv_cols)], w_sem.at[2]),
    ]
    for copy in x_copies + w_copies:
        copy.start()

    def remote(src, dst, ss, rs):
        return pltpu.make_async_remote_copy(src_ref=src, dst_ref=dst, send_sem=ss, recv_sem=rs, device_id=partner, device_id_type=MESH)

    for i in range(x_parts):
        x_copies[i].wait()

        @pl.loop(0, x_rows // ROWS_STEP)
        def _(step, i=i):
            at = pl.ds(pl.multiple_of(i * x_rows + step * ROWS_STEP, ROWS_STEP), ROWS_STEP)
            total = jnp.zeros((ROWS_STEP, 128), jnp.float32)
            for k in range(0, hidden, 128):
                m = xv[at, k:k + 128].astype(jnp.float32)
                total = total + m * m
            ssq[at, :] = total
    pl.semaphore_wait(barrier, 1)
    stats = remote(ssq, ssr, st_ss, st_rs)
    stats.start()
    stats.wait()

    def normalise(start):
        @pl.loop(0, half // ROWS_STEP)
        def _(step):
            at = pl.ds(pl.multiple_of(start + step * ROWS_STEP, ROWS_STEP), ROWS_STEP)
            total = jnp.sum(ssq[at, :] + ssr[at, :], axis=1, keepdims=True)
            inv = lax.rsqrt(total / (2 * hidden) + NORM_EPS)
            for k in range(hidden // 128):
                lanes = slice(k * 128, (k + 1) * 128)
                hbuf[at, lanes] = (xv[at, lanes].astype(jnp.float32) * inv * gain_ref[k:k + 1, :].astype(jnp.float32)).astype(jnp.bfloat16)

    theirs = pl.multiple_of((1 - mx) * half, half)
    mine = pl.multiple_of(mx * half, half)
    normalise(theirs)
    for copy in w_copies:
        copy.wait()
    spans = [(lo, min(lo + 512, width)) for lo in range(0, width, 512)]

    def piece(i, lo, hi):
        return remote(psend.at[:, pl.ds(lo, hi - lo)], precv.at[:, pl.ds(lo, hi - lo)], p_ss.at[i], p_rs.at[i])

    for i, (lo, hi) in enumerate(spans):
        psend[:, lo:hi] = jnp.dot(hbuf[pl.ds(theirs, half), :], wv_all[:, lo:hi], preferred_element_type=jnp.float32).astype(jnp.bfloat16)
        piece(i, lo, hi).start()
    normalise(mine)
    for i, (lo, hi) in enumerate(spans):
        keep[:, lo:hi] = jnp.dot(hbuf[pl.ds(mine, half), :], wv_all[:, lo:hi], preferred_element_type=jnp.float32)
    for i, (lo, hi) in enumerate(spans):
        piece(i, lo, hi).wait_recv()

    def bias_row(ref, h):
        return ref[h:h + 1, :].astype(jnp.float32)

    @pl.loop(0, half // ROWS_STEP)
    def _(step):
        at = pl.ds(pl.multiple_of(step * ROWS_STEP, ROWS_STEP), ROWS_STEP)
        cos_tab, sin_tab = cos_ref[at, :], sin_ref[at, :]
        for h in range(width // HEAD):
            lanes = slice(h * HEAD, (h + 1) * HEAD)
            vals = keep[at, lanes] + precv[at, lanes].astype(jnp.float32)
            if h < q_cols // HEAD:
                out, ref, j, spin = q_out, bq_ref, h, True
            elif h < (q_cols + kv_cols) // HEAD:
                out, ref, j, spin = k_out, bk_ref, h - q_cols // HEAD, True
            else:
                out, ref, j, spin = v_out, bv_ref, h - (q_cols + kv_cols) // HEAD, False
            vals = vals + bias_row(ref, j)
            if spin:
                vals = vals * cos_tab + pltpu.roll(vals, HEAD // 2, 1) * sin_tab
            out[at, j * HEAD:(j + 1) * HEAD] = vals.astype(jnp.bfloat16).astype(jnp.float32)

    for i, (lo, hi) in enumerate(spans):
        piece(i, lo, hi).wait_send()


def head(x_in, gain, b_q, b_k, b_v, cos_tab, sin_tab, w_q, w_k, w_v):
    rows, hidden = x_in.shape
    half = rows // 2
    q_cols, kv_cols = w_q.shape[1], w_k.shape[1]
    width = q_cols + 2 * kv_cols
    whole = pl.BlockSpec(memory_space=pltpu.VMEM)
    hbm = pl.BlockSpec(memory_space=pltpu.HBM)
    bf16, f32 = jnp.bfloat16, jnp.float32
    dma = pltpu.SemaphoreType.DMA
    return pl.pallas_call(
        head_kernel,
        out_shape=(jax.ShapeDtypeStruct((half, q_cols), f32), jax.ShapeDtypeStruct((half, kv_cols), f32), jax.ShapeDtypeStruct((half, kv_cols), f32)),
        in_specs=[hbm] + [whole] * 6 + [hbm] * 3,
        out_specs=(whole, whole, whole),
        scratch_shapes=[
            pltpu.VMEM((rows, hidden), bf16),
            pltpu.VMEM((hidden, width), bf16),
            pltpu.VMEM((rows, hidden), bf16),
            pltpu.VMEM((half, width), f32),
            pltpu.VMEM((half, width), bf16),
            pltpu.VMEM((half, width), bf16),
            pltpu.VMEM((rows, 128), f32),
            pltpu.VMEM((rows, 128), f32),
            dma((4,)), dma((3,)), dma(()), dma(()), dma((4,)), dma((4,)),
        ],
        compiler_params=pltpu.CompilerParams(collective_id=0, has_side_effects=True, vmem_limit_bytes=67043328),
        name="head",
    )(x_in, gain, b_q, b_k, b_v, cos_tab, sin_tab, w_q, w_k, w_v)


def lanes_of(vec):
    return vec.reshape(-1, 128)


def solution(mesh):
    act_spec = P(None, "mx")
    cache_spec = P("mx", None, "my", None)
    in_specs = (act_spec, P("mx"), P("mx"), P("mx"), P("mx", "my"), P("my"), P("mx", "my"), P("my"), P("mx", "my"), P("my"), P("my", "mx"), P("mx", "my"), P("mx", "my"), P("my", "mx"), cache_spec, cache_spec)
    out_specs = (act_spec, cache_spec, cache_spec)

    def local_layer(x_in, seq_lens, gain_attn, gain_mlp, w_q, b_q, w_k, b_k, w_v, b_v, w_o, w_gate, w_up, w_down, k_cache, v_cache):
        half_dim = HEAD // 2
        inv_freq = (ROPE_THETA ** (-2.0 * (np.arange(HEAD) % half_dim) / HEAD)).astype(np.float32)
        sign = np.where(np.arange(HEAD) < half_dim, -1.0, 1.0).astype(np.float32)
        angles = seq_lens.astype(jnp.float32)[:, None] * inv_freq
        cos_tab, sin_tab = jnp.cos(angles), jnp.sin(angles) * sign
        q_rot, k_rot, v_new = head(x_in, lanes_of(gain_attn), lanes_of(b_q), lanes_of(b_k), lanes_of(b_v), cos_tab, sin_tab, w_q, w_k, w_v)
        k_cache_out, v_cache_out, attn_rows = attend(seq_lens, q_rot, k_rot, v_new, k_cache, v_cache)
        x_out = tail(attn_rows, x_in, lanes_of(gain_mlp), w_o, w_gate, w_up, w_down)
        return x_out, k_cache_out, v_cache_out

    return jax.shard_map(local_layer, mesh=mesh, in_specs=in_specs, out_specs=out_specs, check_vma=False)
```

```python
import jax
import jax.numpy as jnp
import numpy as np
from jax import lax
from jax.experimental import pallas as pl
from jax.experimental.pallas import tpu as pltpu
from jax.sharding import PartitionSpec as P

HEAD = 128
NORM_EPS = 1e-6
ROPE_THETA = 1000000.0
SLOT_ROWS = 8
SLOTS = 8
AHEAD = 6
PAD_HEADS = 16
CHUNKS = 2
RING = 8
PIECE = 640
TILE = 256
ROWS_STEP = 16
NORM_ROWS = 64
SERVE = ((5, 11), (9, 14))
HEAD_ROWS = 48
MESH = pl.DeviceIdType.MESH


def attend_kernel(lens, q_hbm, kn_hbm, vn_hbm, kc, vc, ko, vo, out_hbm, kbuf, vbuf, q_ref, kn_ref, vn_ref, out_ref, qs, os, sems, in_sem, out_sem):
    rows = q_ref.shape[0]
    heads = q_ref.shape[1] // HEAD
    flat = kbuf.shape[2]
    blocks = rows // SLOT_ROWS

    def moves(block, slot, inward):
        part = pl.ds(block * SLOT_ROWS, SLOT_ROWS)
        if inward:
            return (pltpu.make_async_copy(kc.at[part], kbuf.at[slot], sems.at[0, slot]),
                    pltpu.make_async_copy(vc.at[part], vbuf.at[slot], sems.at[1, slot]))
        return (pltpu.make_async_copy(kbuf.at[slot], ko.at[part], sems.at[2, slot]),
                pltpu.make_async_copy(vbuf.at[slot], vo.at[part], sems.at[3, slot]))

    for block in range(AHEAD):
        for move in moves(block, block, True):
            move.start()
    loads = [pltpu.make_async_copy(src, dst, in_sem.at[i]) for i, (src, dst) in enumerate(((q_hbm, q_ref), (kn_hbm, kn_ref), (vn_hbm, vn_ref)))]
    for load in loads:
        load.start()
    qs[...] = jnp.zeros_like(qs)

    def put_out(step):
        part = pl.ds(pl.multiple_of(step * 16, 16), 16)
        return pltpu.make_async_copy(out_ref.at[part], out_hbm.at[part], out_sem)

    tile_row = lax.broadcasted_iota(jnp.int32, (PAD_HEADS, HEAD), 0)
    pair_row = lax.broadcasted_iota(jnp.int32, (2 * PAD_HEADS, flat), 0)
    col = lax.broadcasted_iota(jnp.int32, (2 * PAD_HEADS, flat), 1)
    second = pair_row >= PAD_HEADS
    head_of_row = jnp.where(pair_row % PAD_HEADS >= heads // 2, 1, 0)
    col_pos = jnp.where(col % 2 == head_of_row, col // 2, jnp.int32(1 << 20))
    zeros = jnp.zeros((PAD_HEADS, HEAD), jnp.bfloat16)

    def put_row(buf, slot, j, pos, new8):
        base = pl.multiple_of((2 * pos) // 16 * 16, 16)
        off = 2 * pos - base
        tile = buf[slot, j, pl.ds(base, 16), :]
        first = jnp.broadcast_to(new8[j:j + 1, :HEAD], (16, HEAD)).astype(jnp.bfloat16)
        other = jnp.broadcast_to(new8[j:j + 1, HEAD:], (16, HEAD)).astype(jnp.bfloat16)
        tile = jnp.where(tile_row == off, first, jnp.where(tile_row == off + 1, other, tile))
        buf[slot, j, pl.ds(base, 16), :] = tile

    for load in loads:
        load.wait()

    @pl.loop(0, blocks // 2)
    def _(step):
        for half in range(2):
            block = step * 2 + half
            slot = lax.rem(block, SLOTS)
            for move in moves(block, slot, True):
                move.wait()
            rows8 = pl.ds(pl.multiple_of(block * SLOT_ROWS, SLOT_ROWS), SLOT_ROWS)
            kn8, vn8 = kn_ref[rows8, :], vn_ref[rows8, :]
            for h in range(heads):
                qs[pl.ds(h, SLOT_ROWS, stride=PAD_HEADS), :] = q_ref[rows8, h * HEAD:(h + 1) * HEAD]
            for j in range(SLOT_ROWS):
                b = block * SLOT_ROWS + j
                put_row(kbuf, slot, j, lens[b], kn8)
                put_row(vbuf, slot, j, lens[b], vn8)
            pairs = range(0, SLOT_ROWS, 2)
            scores = []
            for j in pairs:
                q0 = qs[j * PAD_HEADS:(j + 1) * PAD_HEADS, :].astype(jnp.bfloat16)
                q1 = qs[(j + 1) * PAD_HEADS:(j + 2) * PAD_HEADS, :].astype(jnp.bfloat16)
                qp = jnp.concatenate([jnp.concatenate([q0, zeros], axis=1), jnp.concatenate([zeros, q1], axis=1)], axis=0)
                kp = jnp.concatenate([kbuf[slot, j], kbuf[slot, j + 1]], axis=1)
                scores.append(lax.dot_general(qp, kp, (((1,), (1,)), ((), ())), preferred_element_type=jnp.float32))
            probs = []
            for i, j in enumerate(pairs):
                b = block * SLOT_ROWS + j
                limit = jnp.where(second, lens[b + 1], lens[b])
                s = jnp.where(col_pos <= limit, scores[i] * HEAD ** -0.5, -jnp.inf)
                e = jnp.exp(s - jnp.max(s, axis=-1, keepdims=True))
                probs.append((e.astype(jnp.bfloat16), jnp.sum(e, axis=-1, keepdims=True)))
            for i, j in enumerate(pairs):
                e, total = probs[i]
                vp = jnp.concatenate([vbuf[slot, j], vbuf[slot, j + 1]], axis=1)
                o = jnp.dot(e, vp, preferred_element_type=jnp.float32)
                at = (half * SLOT_ROWS + j) * PAD_HEADS
                os[at:at + PAD_HEADS, :] = o[:PAD_HEADS, :HEAD] / total[:PAD_HEADS]
                os[at + PAD_HEADS:at + 2 * PAD_HEADS, :] = o[PAD_HEADS:, HEAD:] / total[PAD_HEADS:]
            for move in moves(block, slot, False):
                move.start()

            @pl.when(block + AHEAD < blocks)
            def _():
                later = lax.rem(block + AHEAD, SLOTS)

                @pl.when(block + AHEAD >= SLOTS)
                def _():
                    for move in moves(block + AHEAD - SLOTS, later, False):
                        move.wait()
                for move in moves(block + AHEAD, later, True):
                    move.start()
        for h in range(heads):
            out_ref[pl.ds(pl.multiple_of(step * 16, 16), 16), h * HEAD:(h + 1) * HEAD] = os[pl.ds(h, 16, stride=PAD_HEADS), :].astype(jnp.bfloat16)

        @pl.when(step > 0)
        def _():
            put_out(step - 1).wait()
        put_out(step).start()

    put_out(blocks // 2 - 1).wait()
    for block in range(blocks - SLOTS, blocks):
        for move in moves(block, block % SLOTS, False):
            move.wait()


def attend(lens, q, k_new, v_new, k_cache, v_cache):
    rows, seq, kv, _ = k_cache.shape
    flat = seq * kv
    kc = k_cache.reshape(rows, flat, HEAD)
    vc = v_cache.reshape(rows, flat, HEAD)
    hbm = pl.BlockSpec(memory_space=pltpu.HBM)
    ko, vo, out = pl.pallas_call(
        attend_kernel,
        out_shape=(jax.ShapeDtypeStruct(kc.shape, kc.dtype), jax.ShapeDtypeStruct(vc.shape, vc.dtype), jax.ShapeDtypeStruct(q.shape, jnp.bfloat16)),
        in_specs=[pl.BlockSpec(memory_space=pltpu.SMEM)] + [hbm] * 5,
        out_specs=(hbm, hbm, hbm),
        scratch_shapes=[
            pltpu.VMEM((SLOTS, SLOT_ROWS, flat, HEAD), jnp.bfloat16),
            pltpu.VMEM((SLOTS, SLOT_ROWS, flat, HEAD), jnp.bfloat16),
            pltpu.VMEM(q.shape, q.dtype),
            pltpu.VMEM(k_new.shape, k_new.dtype),
            pltpu.VMEM(v_new.shape, v_new.dtype),
            pltpu.VMEM(q.shape, jnp.bfloat16),
            pltpu.VMEM((SLOT_ROWS * PAD_HEADS, HEAD), jnp.float32),
            pltpu.VMEM((2 * SLOT_ROWS * PAD_HEADS, HEAD), jnp.float32),
            pltpu.SemaphoreType.DMA((4, SLOTS)),
            pltpu.SemaphoreType.DMA((3,)),
            pltpu.SemaphoreType.DMA(()),
        ],
        compiler_params=pltpu.CompilerParams(vmem_limit_bytes=67043328),
        name="attend",
    )(lens, q, k_new, v_new, kc, vc)
    return ko.reshape(k_cache.shape), vo.reshape(v_cache.shape), out


def tail_kernel(attn_hbm, x_hbm, gain_ref, wo_hbm, wg_hbm, wu_hbm, wd_hbm, out_ref,
                attn_all, xown, wo_v, wd_v, ring, sb, rb, keep, mall, hbuf, gsend, grecv, act, ssq, ssr,
                wo_sem, wd_sem, ring_sem, x_sem, ici_ss, ici_rs, gu_ss, gu_rs, act_ss, act_rs, st_ss, st_rs, at_ss, at_rs, at_sem):
    my, mx = lax.axis_index("my"), lax.axis_index("mx")
    row_count, hidden = out_ref.shape
    half_rows = row_count // 2
    sub = half_rows // CHUNKS
    ff = wg_hbm.shape[1]
    steps = (ff // 128 + 1) // 2 * 128 // TILE
    own_w = steps * TILE
    shift = ff - own_w
    per_chunk = 2 * steps
    total_steps = CHUNKS * per_chunk

    def chunk_of(r):
        return lax.rem(my // 2 + r // 2, 2) * 2 + lax.rem(lax.rem(my, 2) + r % 2, 2)

    def device(r):
        return (chunk_of(r), mx)

    partner = (my, 1 - mx)
    first = lambda s: 1 if s == 0 else 2
    second = lambda s: 2 if s == 0 else 1

    def cols(r):
        return pl.ds(pl.multiple_of(chunk_of(r) * PIECE, 128), PIECE)

    barrier = pltpu.get_barrier_semaphore()
    for peer in (device(1), device(2), partner):
        pl.semaphore_signal(barrier, inc=1, device_id=peer, device_id_type=MESH)

    attn_copy = pltpu.make_async_copy(attn_hbm, attn_all.at[mx], at_sem)
    attn_copy.start()
    order = (3, 1, 2, 0)
    wo_copies = {r: pltpu.make_async_copy(wo_hbm.at[:, cols(r)], wo_v.at[:, pl.ds(i * PIECE, PIECE)], wo_sem.at[r]) for i, r in enumerate(order)}
    wd_copies = {r: pltpu.make_async_copy(wd_hbm.at[:, cols(r)], wd_v.at[:, pl.ds(i * PIECE, PIECE)], wd_sem.at[r]) for i, r in enumerate(order)}
    x_copy = pltpu.make_async_copy(x_hbm.at[:, cols(0)], xown, x_sem)
    for r in order:
        wo_copies[r].start()
    x_copy.start()

    def ring_copies(g):
        slot = lax.rem(g, RING)
        at = lax.rem(g, per_chunk)
        mine = at // steps
        side = mine * mx + (1 - mine) * (1 - mx)
        col = pl.multiple_of(side * shift + lax.rem(at, steps) * TILE, 128)
        return (pltpu.make_async_copy(wg_hbm.at[:, pl.ds(col, TILE)], ring.at[slot, :, pl.ds(0, TILE)], ring_sem.at[slot, 0]),
                pltpu.make_async_copy(wu_hbm.at[:, pl.ds(col, TILE)], ring.at[slot, :, pl.ds(TILE, TILE)], ring_sem.at[slot, 1]))

    def remote(src, dst, ss, rs, peer):
        return pltpu.make_async_remote_copy(src_ref=src, dst_ref=dst, send_sem=ss, recv_sem=rs, device_id=peer, device_id_type=MESH)

    def hop(c, s, msg, src, dst, r):
        return remote(src, dst, ici_ss.at[c, s, msg], ici_rs.at[c, s, msg], device(r))

    attn_copy.wait()
    pl.semaphore_wait(barrier, 3)
    attn_msg = remote(attn_all.at[mx], attn_all.at[mx], at_ss, at_rs, partner)
    attn_msg.start()

    def for_rows(count, body, step=ROWS_STEP):
        @pl.loop(0, count // step)
        def _(i):
            body(pl.multiple_of(i * step, step))

    part = sub // 2

    def rs_msg(c, s, base, k):
        if k < 2:
            return hop(c, s, base + k, sb.at[c, s, k], rb.at[c, s, k], first(s))
        rows = pl.ds((k - 2) * part, part)
        return hop(c, s, base + k, sb.at[c, s, 2, rows], rb.at[c, s, 2, rows], second(s))

    def product(c, lhs, weights, copies, base, send):
        waited = []
        for lo in range(0, hidden, 2 * TILE):
            hi = lo + 2 * TILE
            held = [(i, order[i]) for i in range(4) if i * PIECE < hi and (i + 1) * PIECE > lo]
            for _, r in held:
                if copies and r not in waited:
                    waited.append(r)
                    copies[r].wait()
            acc = jnp.dot(lhs, weights[:, lo:hi], preferred_element_type=jnp.float32)
            for i, r in held:
                left, right = max(lo, i * PIECE), min(hi, (i + 1) * PIECE)
                where = slice(left - i * PIECE, right - i * PIECE)
                for s in range(2):
                    piece = acc[s * sub:(s + 1) * sub, left - lo:right - lo]
                    if r == 3 or r == first(s):
                        which = 0 if r == 3 else 1
                        sb[c, s, which, :, where] = piece.astype(jnp.bfloat16)
                        if send and right == (i + 1) * PIECE:
                            rs_msg(c, s, base, which).start()
                    else:
                        keep[c, s, 0 if r == second(s) else 1, :, where] = piece

    def rs_middle(c, base):
        for k in range(2):
            for s in range(2):
                if k == 0:
                    rs_msg(c, s, base, 0).wait_recv()

                def add(at, s=s, k=k):
                    rows = pl.ds(k * part + at, ROWS_STEP)
                    sb[c, s, 2, rows, :] = (keep[c, s, 0, rows, :] + rb[c, s, 0, rows, :].astype(jnp.float32)).astype(jnp.bfloat16)
                for_rows(part, add)
                rs_msg(c, s, base, 2 + k).start()

    def mid_at(c, s, r, k):
        return mall.at[c, chunk_of(r), pl.ds(s * sub + k * part, part), :]

    def out_at(c, s, r, k):
        return out_ref.at[pl.ds(s * half_rows + c * sub + k * part, part), cols(r)]

    def ag_msg(c, s, base, at, j, k):
        src = at(c, s, second(s) if j == 2 else 0, k)
        return hop(c, s, base + 2 * j + k, src, src, second(s) if j == 0 else first(s))

    def finish(c, base, store, at):
        for k in range(2):
            for s in range(2):
                if k == 0:
                    rs_msg(c, s, base, 1).wait_recv()
                rs_msg(c, s, base, 2 + k).wait_recv()

                def add(start, s=s, k=k):
                    rows = pl.ds(k * part + start, ROWS_STEP)
                    total = keep[c, s, 1, rows, :] + rb[c, s, 1, rows, :].astype(jnp.float32) + rb[c, s, 2, rows, :].astype(jnp.float32)
                    store(c, s, k * part + start, total)
                for_rows(part, add)
                ag_msg(c, s, base + 4, at, 0, k).start()
        for k in range(2):
            for s in range(2):
                ag_msg(c, s, base + 4, at, 1, k).start()

    def store_mid(c, s, at, total):
        total = total + xown[pl.ds(s * half_rows + c * sub + at, ROWS_STEP), :].astype(jnp.float32)
        mall[c, my, pl.ds(s * sub + at, ROWS_STEP), :] = total.astype(jnp.bfloat16)

    def store_out(c, s, at, total):
        total = total + mall[c, my, pl.ds(s * sub + at, ROWS_STEP), :].astype(jnp.float32)
        out_ref[pl.ds(s * half_rows + c * sub + at, ROWS_STEP), cols(0)] = total.astype(jnp.bfloat16)

    def finish_mid(c):
        finish(c, 0, store_mid, mid_at)

    def finish_out(c):
        finish(c, 10, store_out, out_at)

    def forward(c, base, at):
        for k in range(2):
            for s in range(2):
                ag_msg(c, s, base, at, 0, k).wait_recv()
                ag_msg(c, s, base, at, 2, k).start()

    def arrive(c, base, at):
        for s in range(2):
            for k in range(2):
                ag_msg(c, s, base, at, 1, k).wait_recv()
                ag_msg(c, s, base, at, 2, k).wait_recv()

    def sent(c, base, at=None):
        for s in range(2):
            if at is None:
                for k in range(4):
                    rs_msg(c, s, base, k).wait_send()
            else:
                for j in range(3):
                    for k in range(2):
                        ag_msg(c, s, base, at, j, k).wait_send()

    def normalise(c):
        def squares(at):
            rows = pl.ds(at, NORM_ROWS)
            total = jnp.zeros((NORM_ROWS, 128), jnp.float32)
            for j in range(4):
                for k in range(0, PIECE, 128):
                    m = mall[c, j, rows, k:k + 128].astype(jnp.float32)
                    total = total + m * m
            ssq[c, rows, :] = total
        for_rows(2 * sub, squares, NORM_ROWS)
        msg = remote(ssq.at[c], ssr.at[c], st_ss.at[c], st_rs.at[c], partner)
        msg.start()
        msg.wait()

        def scale(at):
            rows = pl.ds(at, NORM_ROWS)
            total = jnp.sum(ssq[c, rows, :] + ssr[c, rows, :], axis=1, keepdims=True)
            inv = lax.rsqrt(total / (2 * hidden) + NORM_EPS)
            for j in range(4):
                for k in range(PIECE // 128):
                    tile = j * (PIECE // 128) + k
                    m = mall[c, j, rows, k * 128:(k + 1) * 128].astype(jnp.float32)
                    hbuf[rows, tile * 128:(tile + 1) * 128] = (m * inv * gain_ref[tile:tile + 1, :].astype(jnp.float32)).astype(jnp.bfloat16)
        for_rows(2 * sub, scale, NORM_ROWS)

    def gu_msg(c, t):
        return remote(gsend.at[t], grecv.at[t], gu_ss.at[c, t], gu_rs.at[c, t], partner)

    def tiles(c, mine, lo, hi):
        @pl.loop(lo, hi)
        def _(t):
            g = c * per_chunk + mine * steps + t
            slot = lax.rem(g, RING)
            for copy in ring_copies(g):
                copy.wait()
            if mine:
                gu_msg(c, t).wait_recv()
            acc = jnp.dot(hbuf[...], ring[slot], preferred_element_type=jnp.float32)
            if mine:
                both = acc + grecv[t].astype(jnp.float32)
                gate, up = both[:, :TILE], both[:, TILE:]
                act[:, pl.ds(pl.multiple_of(mx * shift + t * TILE, 128), TILE)] = (gate * jax.nn.sigmoid(gate) * up).astype(jnp.bfloat16)
            else:
                gsend[t] = acc.astype(jnp.bfloat16)
            if not mine:
                gu_msg(c, t).start()

            @pl.when(g + RING < total_steps)
            def _():
                for copy in ring_copies(g + RING):
                    copy.start()

    cut = 3 * TILE

    def act_msg(c, k):
        width = cut if k == 0 else shift - cut
        where = pl.ds(pl.multiple_of(mx * own_w + (0 if k == 0 else cut), 128), width)
        return remote(act.at[:, where], act.at[:, where], act_ss.at[c, k], act_rs.at[c, k], partner)

    def gates_sent(c):
        for t in range(steps):
            gu_msg(c, t).wait_send()

    def attn_lhs(c):
        rows = slice(c * sub, (c + 1) * sub)
        return jnp.concatenate([attn_all[0, rows, :], attn_all[1, rows, :]], axis=0)

    def mlp(c, at, early, late):
        events = sorted([(at[0], 0, early), (at[1], 1, late), (steps + 4, 2, lambda: act_msg(c, 0).start()), (steps, 3, lambda: None), (per_chunk, 4, lambda: None)], key=lambda e: e[:2])
        done = 0
        for pos, _, act_on in events:
            if pos > done:
                mine = done // steps
                tiles(c, mine, done - mine * steps, pos - mine * steps)
                done = pos
            act_on()
        act_msg(c, 1).start()

    attn_msg.wait_recv()
    product(0, attn_lhs(0), wo_v, wo_copies, 0, True)
    for g in range(RING):
        for copy in ring_copies(g):
            copy.start()
    product(1, attn_lhs(1), wo_v, {}, 0, False)
    x_copy.wait()
    for r in order:
        wd_copies[r].start()
    rs_middle(0, 0)
    for s in range(2):
        rs_msg(1, s, 0, 0).start()
    finish_mid(0)
    forward(0, 4, mid_at)
    rs_middle(1, 0)
    for s in range(2):
        rs_msg(1, s, 0, 1).start()
    arrive(0, 4, mid_at)
    normalise(0)
    mlp(0, SERVE[0], lambda: finish_mid(1), lambda: forward(1, 4, mid_at))
    sent(0, 0)
    for k in range(2):
        act_msg(0, k).wait_recv()
    product(0, act[...], wd_v, wd_copies, 10, True)
    gates_sent(0)
    for k in range(2):
        act_msg(0, k).wait_send()
    arrive(1, 4, mid_at)
    normalise(1)
    rs_middle(0, 10)
    mlp(1, SERVE[1], lambda: finish_out(0), lambda: forward(0, 14, out_at))
    sent(1, 0)
    for k in range(2):
        act_msg(1, k).wait_recv()
    product(1, act[...], wd_v, {}, 10, True)
    rs_middle(1, 10)
    arrive(0, 14, out_at)
    finish_out(1)
    forward(1, 14, out_at)
    gates_sent(1)
    for c in range(CHUNKS):
        sent(c, 4, mid_at)
        sent(c, 10)
        if c == 0:
            sent(c, 14, out_at)
    for k in range(2):
        act_msg(1, k).wait_send()
    attn_msg.wait_send()
    arrive(1, 14, out_at)
    sent(1, 14, out_at)


def tail(attn, x_in, gain, w_o, w_gate, w_up, w_down):
    rows, hidden = x_in.shape
    q_width = w_o.shape[0]
    ff = w_gate.shape[1]
    sub = rows // 2 // CHUNKS
    steps = (ff // 128 + 1) // 2 * 128 // TILE
    whole = pl.BlockSpec(memory_space=pltpu.VMEM)
    hbm = pl.BlockSpec(memory_space=pltpu.HBM)
    bf16, f32 = jnp.bfloat16, jnp.float32
    dma = pltpu.SemaphoreType.DMA
    return pl.pallas_call(
        tail_kernel,
        out_shape=jax.ShapeDtypeStruct((rows, hidden), bf16),
        in_specs=[hbm, hbm, whole, hbm, hbm, hbm, hbm],
        out_specs=whole,
        scratch_shapes=[
            pltpu.VMEM((2, rows // 2, q_width), bf16),
            pltpu.VMEM((rows, PIECE), bf16),
            pltpu.VMEM((q_width, hidden), bf16),
            pltpu.VMEM((ff, hidden), bf16),
            pltpu.VMEM((RING, hidden, 2 * TILE), bf16),
            pltpu.VMEM((CHUNKS, 2, 3, sub, PIECE), bf16),
            pltpu.VMEM((CHUNKS, 2, 3, sub, PIECE), bf16),
            pltpu.VMEM((CHUNKS, 2, 2, sub, PIECE), f32),
            pltpu.VMEM((CHUNKS, 4, 2 * sub, PIECE), bf16),
            pltpu.VMEM((2 * sub, hidden), bf16),
            pltpu.VMEM((steps, 2 * sub, 2 * TILE), bf16),
            pltpu.VMEM((steps, 2 * sub, 2 * TILE), bf16),
            pltpu.VMEM((2 * sub, ff), bf16),
            pltpu.VMEM((CHUNKS, 2 * sub, 128), f32),
            pltpu.VMEM((CHUNKS, 2 * sub, 128), f32),
            dma((4,)), dma((4,)), dma((RING, 2)), dma(()),
            dma((CHUNKS, 2, 20)), dma((CHUNKS, 2, 20)),
            dma((CHUNKS, steps)), dma((CHUNKS, steps)),
            dma((CHUNKS, 2)), dma((CHUNKS, 2)),
            dma((CHUNKS,)), dma((CHUNKS,)),
            dma(()), dma(()), dma(()),
        ],
        compiler_params=pltpu.CompilerParams(collective_id=1, has_side_effects=True, vmem_limit_bytes=67043328),
        name="tail",
    )(attn, x_in, gain, w_o, w_gate, w_up, w_down)


def head_kernel(lens, x_hbm, gain_ref, bq_ref, bk_ref, bv_ref, freq_ref, wq_hbm, wk_hbm, wv_hbm, q_out, k_out, v_out,
                xv, wv_all, hbuf, keep, psend, precv, ssq, ssr, cos_ref, sin_ref, x_sem, w_sem, st_ss, st_rs, p_ss, p_rs):
    my, mx = lax.axis_index("my"), lax.axis_index("mx")
    rows, hidden = xv.shape
    half = rows // 2
    q_cols, kv_cols = wq_hbm.shape[1], wk_hbm.shape[1]
    width = q_cols + 2 * kv_cols
    partner = (my, 1 - mx)
    barrier = pltpu.get_barrier_semaphore()
    pl.semaphore_signal(barrier, inc=1, device_id=partner, device_id_type=MESH)

    x_parts = 4
    x_rows = rows // x_parts
    x_copies = [pltpu.make_async_copy(x_hbm.at[pl.ds(i * x_rows, x_rows)], xv.at[pl.ds(i * x_rows, x_rows)], x_sem.at[i]) for i in range(x_parts)]
    w_copies = [
        pltpu.make_async_copy(wq_hbm, wv_all.at[:, pl.ds(0, q_cols)], w_sem.at[0]),
        pltpu.make_async_copy(wk_hbm, wv_all.at[:, pl.ds(q_cols, kv_cols)], w_sem.at[1]),
        pltpu.make_async_copy(wv_hbm, wv_all.at[:, pl.ds(q_cols + kv_cols, kv_cols)], w_sem.at[2]),
    ]
    for copy in x_copies + w_copies:
        copy.start()

    def remote(src, dst, ss, rs):
        return pltpu.make_async_remote_copy(src_ref=src, dst_ref=dst, send_sem=ss, recv_sem=rs, device_id=partner, device_id_type=MESH)

    for i in range(x_parts):
        x_copies[i].wait()

        @pl.loop(0, x_rows // HEAD_ROWS)
        def _(step, i=i):
            at = pl.ds(pl.multiple_of(i * x_rows + step * HEAD_ROWS, HEAD_ROWS), HEAD_ROWS)
            total = jnp.zeros((HEAD_ROWS, 128), jnp.float32)
            for k in range(0, hidden, 128):
                m = xv[at, k:k + 128].astype(jnp.float32)
                total = total + m * m
            ssq[at, :] = total
    pl.semaphore_wait(barrier, 1)
    stats = remote(ssq, ssr, st_ss, st_rs)
    stats.start()
    row_of = lax.broadcasted_iota(jnp.int32, (ROWS_STEP, HEAD), 0)
    lower = lax.broadcasted_iota(jnp.int32, (ROWS_STEP, HEAD), 1) < HEAD // 2

    @pl.loop(0, half // ROWS_STEP)
    def _(step):
        start = pl.multiple_of(step * ROWS_STEP, ROWS_STEP)
        pos = jnp.zeros((ROWS_STEP, HEAD), jnp.int32)
        for i in range(ROWS_STEP):
            pos = jnp.where(row_of == i, lens[start + i], pos)
        angles = pos.astype(jnp.float32) * freq_ref[0:1, :]
        cos_ref[pl.ds(start, ROWS_STEP), :] = jnp.cos(angles)
        sin = jnp.sin(angles)
        sin_ref[pl.ds(start, ROWS_STEP), :] = jnp.where(lower, -sin, sin)

    stats.wait()

    def normalise(start):
        @pl.loop(0, half // NORM_ROWS)
        def _(step):
            at = pl.ds(pl.multiple_of(start + step * NORM_ROWS, NORM_ROWS), NORM_ROWS)
            total = jnp.sum(ssq[at, :] + ssr[at, :], axis=1, keepdims=True)
            inv = lax.rsqrt(total / (2 * hidden) + NORM_EPS)
            for k in range(hidden // 128):
                lanes = slice(k * 128, (k + 1) * 128)
                hbuf[at, lanes] = (xv[at, lanes].astype(jnp.float32) * inv * gain_ref[k:k + 1, :].astype(jnp.float32)).astype(jnp.bfloat16)

    theirs = pl.multiple_of((1 - mx) * half, half)
    mine = pl.multiple_of(mx * half, half)
    normalise(theirs)
    for copy in w_copies:
        copy.wait()
    spans = [(lo, min(lo + 512, width)) for lo in range(0, width, 512)]

    def piece(i, lo, hi):
        return remote(psend.at[:, pl.ds(lo, hi - lo)], precv.at[:, pl.ds(lo, hi - lo)], p_ss.at[i], p_rs.at[i])

    for i, (lo, hi) in enumerate(spans):
        psend[:, lo:hi] = jnp.dot(hbuf[pl.ds(theirs, half), :], wv_all[:, lo:hi], preferred_element_type=jnp.float32).astype(jnp.bfloat16)
        piece(i, lo, hi).start()
    normalise(mine)
    for i, (lo, hi) in enumerate(spans):
        keep[:, lo:hi] = jnp.dot(hbuf[pl.ds(mine, half), :], wv_all[:, lo:hi], preferred_element_type=jnp.float32)
    for i, (lo, hi) in enumerate(spans):
        piece(i, lo, hi).wait_recv()

    def bias_row(ref, h):
        return ref[h:h + 1, :].astype(jnp.float32)

    @pl.loop(0, half // ROWS_STEP)
    def _(step):
        at = pl.ds(pl.multiple_of(step * ROWS_STEP, ROWS_STEP), ROWS_STEP)
        cos_tab, sin_tab = cos_ref[at, :], sin_ref[at, :]
        for h in range(width // HEAD):
            lanes = slice(h * HEAD, (h + 1) * HEAD)
            vals = keep[at, lanes] + precv[at, lanes].astype(jnp.float32)
            if h < q_cols // HEAD:
                out, ref, j, spin = q_out, bq_ref, h, True
            elif h < (q_cols + kv_cols) // HEAD:
                out, ref, j, spin = k_out, bk_ref, h - q_cols // HEAD, True
            else:
                out, ref, j, spin = v_out, bv_ref, h - (q_cols + kv_cols) // HEAD, False
            vals = vals + bias_row(ref, j)
            if spin:
                vals = vals * cos_tab + pltpu.roll(vals, HEAD // 2, 1) * sin_tab
            out[at, j * HEAD:(j + 1) * HEAD] = vals.astype(jnp.bfloat16).astype(jnp.float32)

    for i, (lo, hi) in enumerate(spans):
        piece(i, lo, hi).wait_send()


def head(lens, x_in, gain, b_q, b_k, b_v, freq, w_q, w_k, w_v):
    rows, hidden = x_in.shape
    half = rows // 2
    q_cols, kv_cols = w_q.shape[1], w_k.shape[1]
    width = q_cols + 2 * kv_cols
    whole = pl.BlockSpec(memory_space=pltpu.VMEM)
    hbm = pl.BlockSpec(memory_space=pltpu.HBM)
    bf16, f32 = jnp.bfloat16, jnp.float32
    dma = pltpu.SemaphoreType.DMA
    return pl.pallas_call(
        head_kernel,
        out_shape=(jax.ShapeDtypeStruct((half, q_cols), f32), jax.ShapeDtypeStruct((half, kv_cols), f32), jax.ShapeDtypeStruct((half, kv_cols), f32)),
        in_specs=[pl.BlockSpec(memory_space=pltpu.SMEM), hbm] + [whole] * 5 + [hbm] * 3,
        out_specs=(whole, whole, whole),
        scratch_shapes=[
            pltpu.VMEM((rows, hidden), bf16),
            pltpu.VMEM((hidden, width), bf16),
            pltpu.VMEM((rows, hidden), bf16),
            pltpu.VMEM((half, width), f32),
            pltpu.VMEM((half, width), bf16),
            pltpu.VMEM((half, width), bf16),
            pltpu.VMEM((rows, 128), f32),
            pltpu.VMEM((rows, 128), f32),
            pltpu.VMEM((half, HEAD), f32),
            pltpu.VMEM((half, HEAD), f32),
            dma((4,)), dma((3,)), dma(()), dma(()), dma((4,)), dma((4,)),
        ],
        compiler_params=pltpu.CompilerParams(collective_id=0, has_side_effects=True, vmem_limit_bytes=67043328),
        name="head",
    )(lens, x_in, gain, b_q, b_k, b_v, freq, w_q, w_k, w_v)


def lanes_of(vec):
    return vec.reshape(-1, 128)


def solution(mesh):
    act_spec = P(None, "mx")
    cache_spec = P("mx", None, "my", None)
    in_specs = (act_spec, P("mx"), P("mx"), P("mx"), P("mx", "my"), P("my"), P("mx", "my"), P("my"), P("mx", "my"), P("my"), P("my", "mx"), P("mx", "my"), P("mx", "my"), P("my", "mx"), cache_spec, cache_spec)
    out_specs = (act_spec, cache_spec, cache_spec)

    def local_layer(x_in, seq_lens, gain_attn, gain_mlp, w_q, b_q, w_k, b_k, w_v, b_v, w_o, w_gate, w_up, w_down, k_cache, v_cache):
        half_dim = HEAD // 2
        inv_freq = (ROPE_THETA ** (-2.0 * (np.arange(HEAD) % half_dim) / HEAD)).astype(np.float32)
        freq = jnp.asarray(np.broadcast_to(inv_freq, (8, HEAD)))
        q_rot, k_rot, v_new = head(seq_lens, x_in, lanes_of(gain_attn), lanes_of(b_q), lanes_of(b_k), lanes_of(b_v), freq, w_q, w_k, w_v)
        k_cache_out, v_cache_out, attn_rows = attend(seq_lens, q_rot, k_rot, v_new, k_cache, v_cache)
        x_out = tail(attn_rows, x_in, lanes_of(gain_mlp), w_o, w_gate, w_up, w_down)
        return x_out, k_cache_out, v_cache_out

    return jax.shard_map(local_layer, mesh=mesh, in_specs=in_specs, out_specs=out_specs, check_vma=False)
```

```python
import math

import jax
import jax.numpy as jnp
from jax import lax
from jax.experimental import pallas as pl
from jax.experimental.pallas import tpu as pltpu
from jax.sharding import PartitionSpec as P

HEAD = 128
NORM_EPS = 1e-6
ROPE_THETA = 1000000.0
SLOT_ROWS = 8
SLOTS = 8
AHEAD = 6
PAD_HEADS = 16
CHUNKS = 2
RING = 8
PIECE = 640
TILE = 256
ROWS_STEP = 16
NORM_ROWS = 64
SERVE = ((5, 11), (9, 14))
HEAD_ROWS = 48
MESH = pl.DeviceIdType.MESH


def attend_kernel(lens_hbm, q_hbm, kn_hbm, vn_hbm, kc, vc, ko, vo, out_hbm, kbuf, vbuf, q_ref, kn_ref, vn_ref, out_ref, qs, os, sems, in_sem, out_sem, lens):
    rows = q_ref.shape[0]
    heads = q_ref.shape[1] // HEAD
    flat = kbuf.shape[2]
    blocks = rows // SLOT_ROWS

    def moves(block, slot, inward):
        part = pl.ds(block * SLOT_ROWS, SLOT_ROWS)
        if inward:
            return (pltpu.make_async_copy(kc.at[part], kbuf.at[slot], sems.at[0, slot]),
                    pltpu.make_async_copy(vc.at[part], vbuf.at[slot], sems.at[1, slot]))
        return (pltpu.make_async_copy(kbuf.at[slot], ko.at[part], sems.at[2, slot]),
                pltpu.make_async_copy(vbuf.at[slot], vo.at[part], sems.at[3, slot]))

    loads = [pltpu.make_async_copy(src, dst, in_sem.at[i]) for i, (src, dst) in enumerate(((lens_hbm, lens), (q_hbm, q_ref), (kn_hbm, kn_ref), (vn_hbm, vn_ref)))]
    for load in loads:
        load.start()
    for block in range(AHEAD):
        for move in moves(block, block, True):
            move.start()
    qs[...] = jnp.zeros_like(qs)

    def put_out(step):
        part = pl.ds(pl.multiple_of(step * 16, 16), 16)
        return pltpu.make_async_copy(out_ref.at[part], out_hbm.at[part], out_sem)

    tile_row = lax.broadcasted_iota(jnp.int32, (PAD_HEADS, HEAD), 0)
    pair_row = lax.broadcasted_iota(jnp.int32, (2 * PAD_HEADS, flat), 0)
    col = lax.broadcasted_iota(jnp.int32, (2 * PAD_HEADS, flat), 1)
    second = pair_row >= PAD_HEADS
    head_of_row = jnp.where(pair_row % PAD_HEADS >= heads // 2, 1, 0)
    col_pos = jnp.where(col % 2 == head_of_row, col // 2, jnp.int32(1 << 20))
    zeros = jnp.zeros((PAD_HEADS, HEAD), jnp.bfloat16)

    def put_row(buf, slot, j, pos, new8):
        base = pl.multiple_of((2 * pos) // 16 * 16, 16)
        off = 2 * pos - base
        tile = buf[slot, j, pl.ds(base, 16), :]
        first = jnp.broadcast_to(new8[j:j + 1, :HEAD], (16, HEAD)).astype(jnp.bfloat16)
        other = jnp.broadcast_to(new8[j:j + 1, HEAD:], (16, HEAD)).astype(jnp.bfloat16)
        tile = jnp.where(tile_row == off, first, jnp.where(tile_row == off + 1, other, tile))
        buf[slot, j, pl.ds(base, 16), :] = tile

    for load in loads:
        load.wait()

    @pl.loop(0, blocks // 2)
    def _(step):
        for half in range(2):
            block = step * 2 + half
            slot = lax.rem(block, SLOTS)
            for move in moves(block, slot, True):
                move.wait()
            rows8 = pl.ds(pl.multiple_of(block * SLOT_ROWS, SLOT_ROWS), SLOT_ROWS)
            kn8, vn8 = kn_ref[rows8, :], vn_ref[rows8, :]
            for h in range(heads):
                qs[pl.ds(h, SLOT_ROWS, stride=PAD_HEADS), :] = q_ref[rows8, h * HEAD:(h + 1) * HEAD]
            for j in range(SLOT_ROWS):
                b = block * SLOT_ROWS + j
                put_row(kbuf, slot, j, lens[b], kn8)
                put_row(vbuf, slot, j, lens[b], vn8)
            pairs = range(0, SLOT_ROWS, 2)
            scores = []
            for j in pairs:
                q0 = qs[j * PAD_HEADS:(j + 1) * PAD_HEADS, :].astype(jnp.bfloat16)
                q1 = qs[(j + 1) * PAD_HEADS:(j + 2) * PAD_HEADS, :].astype(jnp.bfloat16)
                qp = jnp.concatenate([jnp.concatenate([q0, zeros], axis=1), jnp.concatenate([zeros, q1], axis=1)], axis=0)
                kp = jnp.concatenate([kbuf[slot, j], kbuf[slot, j + 1]], axis=1)
                scores.append(lax.dot_general(qp, kp, (((1,), (1,)), ((), ())), preferred_element_type=jnp.float32))
            probs = []
            for i, j in enumerate(pairs):
                b = block * SLOT_ROWS + j
                limit = jnp.where(second, lens[b + 1], lens[b])
                s = jnp.where(col_pos <= limit, scores[i] * HEAD ** -0.5, -jnp.inf)
                e = jnp.exp(s - jnp.max(s, axis=-1, keepdims=True))
                probs.append((e.astype(jnp.bfloat16), jnp.sum(e, axis=-1, keepdims=True)))
            for i, j in enumerate(pairs):
                e, total = probs[i]
                vp = jnp.concatenate([vbuf[slot, j], vbuf[slot, j + 1]], axis=1)
                o = jnp.dot(e, vp, preferred_element_type=jnp.float32)
                at = (half * SLOT_ROWS + j) * PAD_HEADS
                os[at:at + PAD_HEADS, :] = o[:PAD_HEADS, :HEAD] / total[:PAD_HEADS]
                os[at + PAD_HEADS:at + 2 * PAD_HEADS, :] = o[PAD_HEADS:, HEAD:] / total[PAD_HEADS:]
            for move in moves(block, slot, False):
                move.start()

            @pl.when(block + AHEAD < blocks)
            def _():
                later = lax.rem(block + AHEAD, SLOTS)

                @pl.when(block + AHEAD >= SLOTS)
                def _():
                    for move in moves(block + AHEAD - SLOTS, later, False):
                        move.wait()
                for move in moves(block + AHEAD, later, True):
                    move.start()
        for h in range(heads):
            out_ref[pl.ds(pl.multiple_of(step * 16, 16), 16), h * HEAD:(h + 1) * HEAD] = os[pl.ds(h, 16, stride=PAD_HEADS), :].astype(jnp.bfloat16)

        @pl.when(step > 0)
        def _():
            put_out(step - 1).wait()
        put_out(step).start()

    put_out(blocks // 2 - 1).wait()
    for block in range(blocks - SLOTS, blocks):
        for move in moves(block, block % SLOTS, False):
            move.wait()


def attend(lens, q, k_new, v_new, k_cache, v_cache):
    rows, seq, kv, _ = k_cache.shape
    flat = seq * kv
    kc = k_cache.reshape(rows, flat, HEAD)
    vc = v_cache.reshape(rows, flat, HEAD)
    hbm = pl.BlockSpec(memory_space=pltpu.HBM)
    ko, vo, out = pl.pallas_call(
        attend_kernel,
        out_shape=(jax.ShapeDtypeStruct(kc.shape, kc.dtype), jax.ShapeDtypeStruct(vc.shape, vc.dtype), jax.ShapeDtypeStruct(q.shape, jnp.bfloat16)),
        in_specs=[hbm] * 6,
        out_specs=(hbm, hbm, hbm),
        scratch_shapes=[
            pltpu.VMEM((SLOTS, SLOT_ROWS, flat, HEAD), jnp.bfloat16),
            pltpu.VMEM((SLOTS, SLOT_ROWS, flat, HEAD), jnp.bfloat16),
            pltpu.VMEM(q.shape, q.dtype),
            pltpu.VMEM(k_new.shape, k_new.dtype),
            pltpu.VMEM(v_new.shape, v_new.dtype),
            pltpu.VMEM(q.shape, jnp.bfloat16),
            pltpu.VMEM((SLOT_ROWS * PAD_HEADS, HEAD), jnp.float32),
            pltpu.VMEM((2 * SLOT_ROWS * PAD_HEADS, HEAD), jnp.float32),
            pltpu.SemaphoreType.DMA((4, SLOTS)),
            pltpu.SemaphoreType.DMA((4,)),
            pltpu.SemaphoreType.DMA(()),
            pltpu.SMEM(lens.shape, lens.dtype),
        ],
        compiler_params=pltpu.CompilerParams(vmem_limit_bytes=67043328),
        name="attend",
    )(lens, q, k_new, v_new, kc, vc)
    return ko.reshape(k_cache.shape), vo.reshape(v_cache.shape), out


def tail_kernel(attn_hbm, x_hbm, gain_hbm, wo_hbm, wg_hbm, wu_hbm, wd_hbm, out_ref,
                attn_all, xown, wo_v, wd_v, ring, sb, rb, keep, mall, hbuf, gsend, grecv, act, ssq, ssr,
                wo_sem, wd_sem, ring_sem, x_sem, ici_ss, ici_rs, gu_ss, gu_rs, act_ss, act_rs, st_ss, st_rs, at_ss, at_rs, at_sem, gain_ref, gain_sem):
    my, mx = lax.axis_index("my"), lax.axis_index("mx")
    row_count, hidden = out_ref.shape
    half_rows = row_count // 2
    sub = half_rows // CHUNKS
    ff = wg_hbm.shape[1]
    steps = (ff // 128 + 1) // 2 * 128 // TILE
    own_w = steps * TILE
    shift = ff - own_w
    per_chunk = 2 * steps
    total_steps = CHUNKS * per_chunk

    def chunk_of(r):
        return lax.rem(my // 2 + r // 2, 2) * 2 + lax.rem(lax.rem(my, 2) + r % 2, 2)

    def device(r):
        return (chunk_of(r), mx)

    partner = (my, 1 - mx)
    first = lambda s: 1 if s == 0 else 2
    second = lambda s: 2 if s == 0 else 1

    def cols(r):
        return pl.ds(pl.multiple_of(chunk_of(r) * PIECE, 128), PIECE)

    barrier = pltpu.get_barrier_semaphore()
    for peer in (device(1), device(2), partner):
        pl.semaphore_signal(barrier, inc=1, device_id=peer, device_id_type=MESH)

    attn_copy = pltpu.make_async_copy(attn_hbm, attn_all.at[mx], at_sem)
    attn_copy.start()
    order = (3, 1, 2, 0)
    wo_copies = {r: pltpu.make_async_copy(wo_hbm.at[:, cols(r)], wo_v.at[:, pl.ds(i * PIECE, PIECE)], wo_sem.at[r]) for i, r in enumerate(order)}
    wd_copies = {r: pltpu.make_async_copy(wd_hbm.at[:, cols(r)], wd_v.at[:, pl.ds(i * PIECE, PIECE)], wd_sem.at[r]) for i, r in enumerate(order)}
    x_copy = pltpu.make_async_copy(x_hbm.at[:, cols(0)], xown, x_sem)
    for r in order:
        wo_copies[r].start()
    x_copy.start()
    gain_copy = pltpu.make_async_copy(gain_hbm, gain_ref, gain_sem)
    gain_copy.start()

    def ring_copies(g):
        slot = lax.rem(g, RING)
        at = lax.rem(g, per_chunk)
        mine = at // steps
        side = mine * mx + (1 - mine) * (1 - mx)
        col = pl.multiple_of(side * shift + lax.rem(at, steps) * TILE, 128)
        return (pltpu.make_async_copy(wg_hbm.at[:, pl.ds(col, TILE)], ring.at[slot, :, pl.ds(0, TILE)], ring_sem.at[slot, 0]),
                pltpu.make_async_copy(wu_hbm.at[:, pl.ds(col, TILE)], ring.at[slot, :, pl.ds(TILE, TILE)], ring_sem.at[slot, 1]))

    def remote(src, dst, ss, rs, peer):
        return pltpu.make_async_remote_copy(src_ref=src, dst_ref=dst, send_sem=ss, recv_sem=rs, device_id=peer, device_id_type=MESH)

    def hop(c, s, msg, src, dst, r):
        return remote(src, dst, ici_ss.at[c, s, msg], ici_rs.at[c, s, msg], device(r))

    attn_copy.wait()
    pl.semaphore_wait(barrier, 3)
    attn_msg = remote(attn_all.at[mx], attn_all.at[mx], at_ss, at_rs, partner)
    attn_msg.start()

    def for_rows(count, body, step=ROWS_STEP):
        @pl.loop(0, count // step)
        def _(i):
            body(pl.multiple_of(i * step, step))

    part = sub // 2

    def rs_msg(c, s, base, k):
        if k < 2:
            return hop(c, s, base + k, sb.at[c, s, k], rb.at[c, s, k], first(s))
        rows = pl.ds((k - 2) * part, part)
        return hop(c, s, base + k, sb.at[c, s, 2, rows], rb.at[c, s, 2, rows], second(s))

    def product(c, lhs, weights, copies, base, send):
        waited = []
        for lo in range(0, hidden, 2 * TILE):
            hi = lo + 2 * TILE
            held = [(i, order[i]) for i in range(4) if i * PIECE < hi and (i + 1) * PIECE > lo]
            for _, r in held:
                if copies and r not in waited:
                    waited.append(r)
                    copies[r].wait()
            acc = jnp.dot(lhs, weights[:, lo:hi], preferred_element_type=jnp.float32)
            for i, r in held:
                left, right = max(lo, i * PIECE), min(hi, (i + 1) * PIECE)
                where = slice(left - i * PIECE, right - i * PIECE)
                for s in range(2):
                    piece = acc[s * sub:(s + 1) * sub, left - lo:right - lo]
                    if r == 3 or r == first(s):
                        which = 0 if r == 3 else 1
                        sb[c, s, which, :, where] = piece.astype(jnp.bfloat16)
                        if send and right == (i + 1) * PIECE:
                            rs_msg(c, s, base, which).start()
                    else:
                        keep[c, s, 0 if r == second(s) else 1, :, where] = piece

    def rs_middle(c, base):
        for k in range(2):
            for s in range(2):
                if k == 0:
                    rs_msg(c, s, base, 0).wait_recv()

                def add(at, s=s, k=k):
                    rows = pl.ds(k * part + at, ROWS_STEP)
                    sb[c, s, 2, rows, :] = (keep[c, s, 0, rows, :] + rb[c, s, 0, rows, :].astype(jnp.float32)).astype(jnp.bfloat16)
                for_rows(part, add)
                rs_msg(c, s, base, 2 + k).start()

    def mid_at(c, s, r, k):
        return mall.at[c, chunk_of(r), pl.ds(s * sub + k * part, part), :]

    def out_at(c, s, r, k):
        return out_ref.at[pl.ds(s * half_rows + c * sub + k * part, part), cols(r)]

    def ag_msg(c, s, base, at, j, k):
        src = at(c, s, second(s) if j == 2 else 0, k)
        return hop(c, s, base + 2 * j + k, src, src, second(s) if j == 0 else first(s))

    def finish(c, base, store, at):
        for k in range(2):
            for s in range(2):
                if k == 0:
                    rs_msg(c, s, base, 1).wait_recv()
                rs_msg(c, s, base, 2 + k).wait_recv()

                def add(start, s=s, k=k):
                    rows = pl.ds(k * part + start, ROWS_STEP)
                    total = keep[c, s, 1, rows, :] + rb[c, s, 1, rows, :].astype(jnp.float32) + rb[c, s, 2, rows, :].astype(jnp.float32)
                    store(c, s, k * part + start, total)
                for_rows(part, add)
                ag_msg(c, s, base + 4, at, 0, k).start()
        for k in range(2):
            for s in range(2):
                ag_msg(c, s, base + 4, at, 1, k).start()

    def store_mid(c, s, at, total):
        total = total + xown[pl.ds(s * half_rows + c * sub + at, ROWS_STEP), :].astype(jnp.float32)
        mall[c, my, pl.ds(s * sub + at, ROWS_STEP), :] = total.astype(jnp.bfloat16)

    def store_out(c, s, at, total):
        total = total + mall[c, my, pl.ds(s * sub + at, ROWS_STEP), :].astype(jnp.float32)
        out_ref[pl.ds(s * half_rows + c * sub + at, ROWS_STEP), cols(0)] = total.astype(jnp.bfloat16)

    def finish_mid(c):
        finish(c, 0, store_mid, mid_at)

    def finish_out(c):
        finish(c, 10, store_out, out_at)

    def forward(c, base, at):
        for k in range(2):
            for s in range(2):
                ag_msg(c, s, base, at, 0, k).wait_recv()
                ag_msg(c, s, base, at, 2, k).start()

    def arrive(c, base, at):
        for s in range(2):
            for k in range(2):
                ag_msg(c, s, base, at, 1, k).wait_recv()
                ag_msg(c, s, base, at, 2, k).wait_recv()

    def sent(c, base, at=None):
        for s in range(2):
            if at is None:
                for k in range(4):
                    rs_msg(c, s, base, k).wait_send()
            else:
                for j in range(3):
                    for k in range(2):
                        ag_msg(c, s, base, at, j, k).wait_send()

    def normalise(c):
        def squares(at):
            rows = pl.ds(at, NORM_ROWS)
            total = jnp.zeros((NORM_ROWS, 128), jnp.float32)
            for j in range(4):
                for k in range(0, PIECE, 128):
                    m = mall[c, j, rows, k:k + 128].astype(jnp.float32)
                    total = total + m * m
            ssq[c, rows, :] = total
        for_rows(2 * sub, squares, NORM_ROWS)
        msg = remote(ssq.at[c], ssr.at[c], st_ss.at[c], st_rs.at[c], partner)
        msg.start()
        msg.wait()

        def scale(at):
            rows = pl.ds(at, NORM_ROWS)
            total = jnp.sum(ssq[c, rows, :] + ssr[c, rows, :], axis=1, keepdims=True)
            inv = lax.rsqrt(total / (2 * hidden) + NORM_EPS)
            for j in range(4):
                for k in range(PIECE // 128):
                    tile = j * (PIECE // 128) + k
                    m = mall[c, j, rows, k * 128:(k + 1) * 128].astype(jnp.float32)
                    hbuf[rows, tile * 128:(tile + 1) * 128] = (m * inv * gain_ref[tile:tile + 1, :].astype(jnp.float32)).astype(jnp.bfloat16)
        for_rows(2 * sub, scale, NORM_ROWS)

    def gu_msg(c, t):
        return remote(gsend.at[t], grecv.at[t], gu_ss.at[c, t], gu_rs.at[c, t], partner)

    def tiles(c, mine, lo, hi):
        @pl.loop(lo, hi)
        def _(t):
            g = c * per_chunk + mine * steps + t
            slot = lax.rem(g, RING)
            for copy in ring_copies(g):
                copy.wait()
            if mine:
                gu_msg(c, t).wait_recv()
            acc = jnp.dot(hbuf[...], ring[slot], preferred_element_type=jnp.float32)
            if mine:
                both = acc + grecv[t].astype(jnp.float32)
                gate, up = both[:, :TILE], both[:, TILE:]
                act[:, pl.ds(pl.multiple_of(mx * shift + t * TILE, 128), TILE)] = (gate * jax.nn.sigmoid(gate) * up).astype(jnp.bfloat16)
            else:
                gsend[t] = acc.astype(jnp.bfloat16)
            if not mine:
                gu_msg(c, t).start()

            @pl.when(g + RING < total_steps)
            def _():
                for copy in ring_copies(g + RING):
                    copy.start()

    cut = 3 * TILE

    def act_msg(c, k):
        width = cut if k == 0 else shift - cut
        where = pl.ds(pl.multiple_of(mx * own_w + (0 if k == 0 else cut), 128), width)
        return remote(act.at[:, where], act.at[:, where], act_ss.at[c, k], act_rs.at[c, k], partner)

    def gates_sent(c):
        for t in range(steps):
            gu_msg(c, t).wait_send()

    def attn_lhs(c):
        rows = slice(c * sub, (c + 1) * sub)
        return jnp.concatenate([attn_all[0, rows, :], attn_all[1, rows, :]], axis=0)

    def mlp(c, at, early, late):
        events = sorted([(at[0], 0, early), (at[1], 1, late), (steps + 4, 2, lambda: act_msg(c, 0).start()), (steps, 3, lambda: None), (per_chunk, 4, lambda: None)], key=lambda e: e[:2])
        done = 0
        for pos, _, act_on in events:
            if pos > done:
                mine = done // steps
                tiles(c, mine, done - mine * steps, pos - mine * steps)
                done = pos
            act_on()
        act_msg(c, 1).start()

    attn_msg.wait_recv()
    product(0, attn_lhs(0), wo_v, wo_copies, 0, True)
    for g in range(RING):
        for copy in ring_copies(g):
            copy.start()
    product(1, attn_lhs(1), wo_v, {}, 0, False)
    x_copy.wait()
    gain_copy.wait()
    for r in order:
        wd_copies[r].start()
    rs_middle(0, 0)
    for s in range(2):
        rs_msg(1, s, 0, 0).start()
    finish_mid(0)
    forward(0, 4, mid_at)
    rs_middle(1, 0)
    for s in range(2):
        rs_msg(1, s, 0, 1).start()
    arrive(0, 4, mid_at)
    normalise(0)
    mlp(0, SERVE[0], lambda: finish_mid(1), lambda: forward(1, 4, mid_at))
    sent(0, 0)
    for k in range(2):
        act_msg(0, k).wait_recv()
    product(0, act[...], wd_v, wd_copies, 10, True)
    gates_sent(0)
    for k in range(2):
        act_msg(0, k).wait_send()
    arrive(1, 4, mid_at)
    normalise(1)
    rs_middle(0, 10)
    mlp(1, SERVE[1], lambda: finish_out(0), lambda: forward(0, 14, out_at))
    sent(1, 0)
    for k in range(2):
        act_msg(1, k).wait_recv()
    product(1, act[...], wd_v, {}, 10, True)
    rs_middle(1, 10)
    arrive(0, 14, out_at)
    finish_out(1)
    forward(1, 14, out_at)
    gates_sent(1)
    for c in range(CHUNKS):
        sent(c, 4, mid_at)
        sent(c, 10)
        if c == 0:
            sent(c, 14, out_at)
    for k in range(2):
        act_msg(1, k).wait_send()
    attn_msg.wait_send()
    arrive(1, 14, out_at)
    sent(1, 14, out_at)


def tail(attn, x_in, gain, w_o, w_gate, w_up, w_down):
    rows, hidden = x_in.shape
    q_width = w_o.shape[0]
    ff = w_gate.shape[1]
    sub = rows // 2 // CHUNKS
    steps = (ff // 128 + 1) // 2 * 128 // TILE
    whole = pl.BlockSpec(memory_space=pltpu.VMEM)
    hbm = pl.BlockSpec(memory_space=pltpu.HBM)
    bf16, f32 = jnp.bfloat16, jnp.float32
    dma = pltpu.SemaphoreType.DMA
    return pl.pallas_call(
        tail_kernel,
        out_shape=jax.ShapeDtypeStruct((rows, hidden), bf16),
        in_specs=[hbm] * 7,
        out_specs=whole,
        scratch_shapes=[
            pltpu.VMEM((2, rows // 2, q_width), bf16),
            pltpu.VMEM((rows, PIECE), bf16),
            pltpu.VMEM((q_width, hidden), bf16),
            pltpu.VMEM((ff, hidden), bf16),
            pltpu.VMEM((RING, hidden, 2 * TILE), bf16),
            pltpu.VMEM((CHUNKS, 2, 3, sub, PIECE), bf16),
            pltpu.VMEM((CHUNKS, 2, 3, sub, PIECE), bf16),
            pltpu.VMEM((CHUNKS, 2, 2, sub, PIECE), f32),
            pltpu.VMEM((CHUNKS, 4, 2 * sub, PIECE), bf16),
            pltpu.VMEM((2 * sub, hidden), bf16),
            pltpu.VMEM((steps, 2 * sub, 2 * TILE), bf16),
            pltpu.VMEM((steps, 2 * sub, 2 * TILE), bf16),
            pltpu.VMEM((2 * sub, ff), bf16),
            pltpu.VMEM((CHUNKS, 2 * sub, 128), f32),
            pltpu.VMEM((CHUNKS, 2 * sub, 128), f32),
            dma((4,)), dma((4,)), dma((RING, 2)), dma(()),
            dma((CHUNKS, 2, 20)), dma((CHUNKS, 2, 20)),
            dma((CHUNKS, steps)), dma((CHUNKS, steps)),
            dma((CHUNKS, 2)), dma((CHUNKS, 2)),
            dma((CHUNKS,)), dma((CHUNKS,)),
            dma(()), dma(()), dma(()),
            pltpu.VMEM(gain.shape, bf16), dma(()),
        ],
        compiler_params=pltpu.CompilerParams(collective_id=1, has_side_effects=True, vmem_limit_bytes=67043328),
        name="tail",
    )(attn, x_in, gain, w_o, w_gate, w_up, w_down)


def head_kernel(lens_hbm, x_hbm, gain_hbm, bq_hbm, bk_hbm, bv_hbm, wq_hbm, wk_hbm, wv_hbm, q_out, k_out, v_out,
                xv, wv_all, hbuf, keep, psend, precv, ssq, ssr, cos_ref, sin_ref, x_sem, w_sem, st_ss, st_rs, p_ss, p_rs, lens, gain_ref, bq_ref, bk_ref, bv_ref, small_sem):
    my, mx = lax.axis_index("my"), lax.axis_index("mx")
    rows, hidden = xv.shape
    half = rows // 2
    q_cols, kv_cols = wq_hbm.shape[1], wk_hbm.shape[1]
    width = q_cols + 2 * kv_cols
    partner = (my, 1 - mx)
    barrier = pltpu.get_barrier_semaphore()
    pl.semaphore_signal(barrier, inc=1, device_id=partner, device_id_type=MESH)

    x_parts = 4
    x_rows = rows // x_parts
    x_copies = [pltpu.make_async_copy(x_hbm.at[pl.ds(i * x_rows, x_rows)], xv.at[pl.ds(i * x_rows, x_rows)], x_sem.at[i]) for i in range(x_parts)]
    w_copies = [
        pltpu.make_async_copy(wq_hbm, wv_all.at[:, pl.ds(0, q_cols)], w_sem.at[0]),
        pltpu.make_async_copy(wk_hbm, wv_all.at[:, pl.ds(q_cols, kv_cols)], w_sem.at[1]),
        pltpu.make_async_copy(wv_hbm, wv_all.at[:, pl.ds(q_cols + kv_cols, kv_cols)], w_sem.at[2]),
    ]
    small = [pltpu.make_async_copy(src, dst, small_sem.at[i]) for i, (src, dst) in enumerate(((lens_hbm, lens), (gain_hbm, gain_ref), (bq_hbm, bq_ref), (bk_hbm, bk_ref), (bv_hbm, bv_ref)))]
    for copy in x_copies + small + w_copies:
        copy.start()

    def remote(src, dst, ss, rs):
        return pltpu.make_async_remote_copy(src_ref=src, dst_ref=dst, send_sem=ss, recv_sem=rs, device_id=partner, device_id_type=MESH)

    for i in range(x_parts):
        x_copies[i].wait()

        @pl.loop(0, x_rows // HEAD_ROWS)
        def _(step, i=i):
            at = pl.ds(pl.multiple_of(i * x_rows + step * HEAD_ROWS, HEAD_ROWS), HEAD_ROWS)
            total = jnp.zeros((HEAD_ROWS, 128), jnp.float32)
            for k in range(0, hidden, 128):
                m = xv[at, k:k + 128].astype(jnp.float32)
                total = total + m * m
            ssq[at, :] = total
    pl.semaphore_wait(barrier, 1)
    stats = remote(ssq, ssr, st_ss, st_rs)
    stats.start()
    for copy in small:
        copy.wait()
    row_of = lax.broadcasted_iota(jnp.int32, (ROWS_STEP, HEAD), 0)
    lane = lax.broadcasted_iota(jnp.int32, (ROWS_STEP, HEAD), 1)
    lower = lane < HEAD // 2
    freq = jnp.exp(lax.rem(lane, HEAD // 2).astype(jnp.float32) * (-2.0 * math.log(ROPE_THETA) / HEAD))

    @pl.loop(0, half // ROWS_STEP)
    def _(step):
        start = pl.multiple_of(step * ROWS_STEP, ROWS_STEP)
        pos = jnp.zeros((ROWS_STEP, HEAD), jnp.int32)
        for i in range(ROWS_STEP):
            pos = jnp.where(row_of == i, lens[start + i], pos)
        angles = pos.astype(jnp.float32) * freq
        cos_ref[pl.ds(start, ROWS_STEP), :] = jnp.cos(angles)
        sin = jnp.sin(angles)
        sin_ref[pl.ds(start, ROWS_STEP), :] = jnp.where(lower, -sin, sin)

    stats.wait()

    def normalise(start):
        @pl.loop(0, half // NORM_ROWS)
        def _(step):
            at = pl.ds(pl.multiple_of(start + step * NORM_ROWS, NORM_ROWS), NORM_ROWS)
            total = jnp.sum(ssq[at, :] + ssr[at, :], axis=1, keepdims=True)
            inv = lax.rsqrt(total / (2 * hidden) + NORM_EPS)
            for k in range(hidden // 128):
                lanes = slice(k * 128, (k + 1) * 128)
                hbuf[at, lanes] = (xv[at, lanes].astype(jnp.float32) * inv * gain_ref[k:k + 1, :].astype(jnp.float32)).astype(jnp.bfloat16)

    theirs = pl.multiple_of((1 - mx) * half, half)
    mine = pl.multiple_of(mx * half, half)
    normalise(theirs)
    for copy in w_copies:
        copy.wait()
    spans = [(lo, min(lo + 512, width)) for lo in range(0, width, 512)]

    def piece(i, lo, hi):
        return remote(psend.at[:, pl.ds(lo, hi - lo)], precv.at[:, pl.ds(lo, hi - lo)], p_ss.at[i], p_rs.at[i])

    for i, (lo, hi) in enumerate(spans):
        psend[:, lo:hi] = jnp.dot(hbuf[pl.ds(theirs, half), :], wv_all[:, lo:hi], preferred_element_type=jnp.float32).astype(jnp.bfloat16)
        piece(i, lo, hi).start()
    normalise(mine)
    for i, (lo, hi) in enumerate(spans):
        keep[:, lo:hi] = jnp.dot(hbuf[pl.ds(mine, half), :], wv_all[:, lo:hi], preferred_element_type=jnp.float32)
    for i, (lo, hi) in enumerate(spans):
        piece(i, lo, hi).wait_recv()

    def bias_row(ref, h):
        return ref[h:h + 1, :].astype(jnp.float32)

    @pl.loop(0, half // ROWS_STEP)
    def _(step):
        at = pl.ds(pl.multiple_of(step * ROWS_STEP, ROWS_STEP), ROWS_STEP)
        cos_tab, sin_tab = cos_ref[at, :], sin_ref[at, :]
        for h in range(width // HEAD):
            lanes = slice(h * HEAD, (h + 1) * HEAD)
            vals = keep[at, lanes] + precv[at, lanes].astype(jnp.float32)
            if h < q_cols // HEAD:
                out, ref, j, spin = q_out, bq_ref, h, True
            elif h < (q_cols + kv_cols) // HEAD:
                out, ref, j, spin = k_out, bk_ref, h - q_cols // HEAD, True
            else:
                out, ref, j, spin = v_out, bv_ref, h - (q_cols + kv_cols) // HEAD, False
            vals = vals + bias_row(ref, j)
            if spin:
                vals = vals * cos_tab + pltpu.roll(vals, HEAD // 2, 1) * sin_tab
            out[at, j * HEAD:(j + 1) * HEAD] = vals.astype(jnp.bfloat16).astype(jnp.float32)

    for i, (lo, hi) in enumerate(spans):
        piece(i, lo, hi).wait_send()


def head(lens, x_in, gain, b_q, b_k, b_v, w_q, w_k, w_v):
    rows, hidden = x_in.shape
    half = rows // 2
    q_cols, kv_cols = w_q.shape[1], w_k.shape[1]
    width = q_cols + 2 * kv_cols
    whole = pl.BlockSpec(memory_space=pltpu.VMEM)
    hbm = pl.BlockSpec(memory_space=pltpu.HBM)
    bf16, f32 = jnp.bfloat16, jnp.float32
    dma = pltpu.SemaphoreType.DMA
    return pl.pallas_call(
        head_kernel,
        out_shape=(jax.ShapeDtypeStruct((half, q_cols), f32), jax.ShapeDtypeStruct((half, kv_cols), f32), jax.ShapeDtypeStruct((half, kv_cols), f32)),
        in_specs=[hbm] * 9,
        out_specs=(whole, whole, whole),
        scratch_shapes=[
            pltpu.VMEM((rows, hidden), bf16),
            pltpu.VMEM((hidden, width), bf16),
            pltpu.VMEM((rows, hidden), bf16),
            pltpu.VMEM((half, width), f32),
            pltpu.VMEM((half, width), bf16),
            pltpu.VMEM((half, width), bf16),
            pltpu.VMEM((rows, 128), f32),
            pltpu.VMEM((rows, 128), f32),
            pltpu.VMEM((half, HEAD), f32),
            pltpu.VMEM((half, HEAD), f32),
            dma((4,)), dma((3,)), dma(()), dma(()), dma((4,)), dma((4,)),
            pltpu.SMEM(lens.shape, lens.dtype),
            pltpu.VMEM(gain.shape, bf16), pltpu.VMEM(b_q.shape, bf16), pltpu.VMEM(b_k.shape, bf16), pltpu.VMEM(b_v.shape, bf16),
            dma((5,)),
        ],
        compiler_params=pltpu.CompilerParams(collective_id=0, has_side_effects=True, vmem_limit_bytes=67043328),
        name="head",
    )(lens, x_in, gain, b_q, b_k, b_v, w_q, w_k, w_v)


def lanes_of(vec):
    return vec.reshape(-1, 128)


def solution(mesh):
    act_spec = P(None, "mx")
    cache_spec = P("mx", None, "my", None)
    in_specs = (act_spec, P("mx"), P("mx"), P("mx"), P("mx", "my"), P("my"), P("mx", "my"), P("my"), P("mx", "my"), P("my"), P("my", "mx"), P("mx", "my"), P("mx", "my"), P("my", "mx"), cache_spec, cache_spec)
    out_specs = (act_spec, cache_spec, cache_spec)

    def local_layer(x_in, seq_lens, gain_attn, gain_mlp, w_q, b_q, w_k, b_k, w_v, b_v, w_o, w_gate, w_up, w_down, k_cache, v_cache):
        q_rot, k_rot, v_new = head(seq_lens, x_in, lanes_of(gain_attn), lanes_of(b_q), lanes_of(b_k), lanes_of(b_v), w_q, w_k, w_v)
        k_cache_out, v_cache_out, attn_rows = attend(seq_lens, q_rot, k_rot, v_new, k_cache, v_cache)
        x_out = tail(attn_rows, x_in, lanes_of(gain_mlp), w_o, w_gate, w_up, w_down)
        return x_out, k_cache_out, v_cache_out

    return jax.shard_map(local_layer, mesh=mesh, in_specs=in_specs, out_specs=out_specs, check_vma=False)
```

```python
import math

import jax
import jax.numpy as jnp
from jax import lax
from jax.experimental import pallas as pl
from jax.experimental.pallas import tpu as pltpu
from jax.sharding import PartitionSpec as P

HEAD = 128
NORM_EPS = 1e-6
ROPE_THETA = 1000000.0
SLOT_ROWS = 8
SLOTS = 8
AHEAD = 6
PAD_HEADS = 16
CHUNKS = 2
RING = 8
PIECE = 640
TILE = 256
ROWS_STEP = 16
NORM_ROWS = 64
SERVE = ((5, 11), (7, 13))
HEAD_ROWS = 48
MESH = pl.DeviceIdType.MESH


def attend_kernel(lens_hbm, q_hbm, kn_hbm, vn_hbm, kc, vc, ko, vo, out_hbm, kbuf, vbuf, q_ref, kn_ref, vn_ref, out_ref, qs, os, sems, in_sem, out_sem, lens):
    rows = q_ref.shape[0]
    heads = q_ref.shape[1] // HEAD
    flat = kbuf.shape[2]
    blocks = rows // SLOT_ROWS

    def moves(block, slot, inward):
        part = pl.ds(block * SLOT_ROWS, SLOT_ROWS)
        if inward:
            return (pltpu.make_async_copy(kc.at[part], kbuf.at[slot], sems.at[0, slot]),
                    pltpu.make_async_copy(vc.at[part], vbuf.at[slot], sems.at[1, slot]))
        return (pltpu.make_async_copy(kbuf.at[slot], ko.at[part], sems.at[2, slot]),
                pltpu.make_async_copy(vbuf.at[slot], vo.at[part], sems.at[3, slot]))

    loads = [pltpu.make_async_copy(src, dst, in_sem.at[i]) for i, (src, dst) in enumerate(((lens_hbm, lens), (q_hbm, q_ref), (kn_hbm, kn_ref), (vn_hbm, vn_ref)))]
    for load in loads:
        load.start()
    for block in range(AHEAD):
        for move in moves(block, block, True):
            move.start()
    qs[...] = jnp.zeros_like(qs)

    def put_out(step):
        part = pl.ds(pl.multiple_of(step * 16, 16), 16)
        return pltpu.make_async_copy(out_ref.at[part], out_hbm.at[part], out_sem)

    tile_row = lax.broadcasted_iota(jnp.int32, (PAD_HEADS, HEAD), 0)
    pair_row = lax.broadcasted_iota(jnp.int32, (2 * PAD_HEADS, flat), 0)
    col = lax.broadcasted_iota(jnp.int32, (2 * PAD_HEADS, flat), 1)
    second = pair_row >= PAD_HEADS
    head_of_row = jnp.where(pair_row % PAD_HEADS >= heads // 2, 1, 0)
    col_pos = jnp.where(col % 2 == head_of_row, col // 2, jnp.int32(1 << 20))
    zeros = jnp.zeros((PAD_HEADS, HEAD), jnp.bfloat16)

    def put_row(buf, slot, j, pos, new8):
        base = pl.multiple_of((2 * pos) // 16 * 16, 16)
        off = 2 * pos - base
        tile = buf[slot, j, pl.ds(base, 16), :]
        first = jnp.broadcast_to(new8[j:j + 1, :HEAD], (16, HEAD)).astype(jnp.bfloat16)
        other = jnp.broadcast_to(new8[j:j + 1, HEAD:], (16, HEAD)).astype(jnp.bfloat16)
        tile = jnp.where(tile_row == off, first, jnp.where(tile_row == off + 1, other, tile))
        buf[slot, j, pl.ds(base, 16), :] = tile

    for load in loads:
        load.wait()

    @pl.loop(0, blocks // 2)
    def _(step):
        for half in range(2):
            block = step * 2 + half
            slot = lax.rem(block, SLOTS)
            for move in moves(block, slot, True):
                move.wait()
            rows8 = pl.ds(pl.multiple_of(block * SLOT_ROWS, SLOT_ROWS), SLOT_ROWS)
            kn8, vn8 = kn_ref[rows8, :], vn_ref[rows8, :]
            for h in range(heads):
                qs[pl.ds(h, SLOT_ROWS, stride=PAD_HEADS), :] = q_ref[rows8, h * HEAD:(h + 1) * HEAD]
            for j in range(SLOT_ROWS):
                b = block * SLOT_ROWS + j
                put_row(kbuf, slot, j, lens[b], kn8)
                put_row(vbuf, slot, j, lens[b], vn8)
            pairs = range(0, SLOT_ROWS, 2)
            scores = []
            for j in pairs:
                q0 = qs[j * PAD_HEADS:(j + 1) * PAD_HEADS, :].astype(jnp.bfloat16)
                q1 = qs[(j + 1) * PAD_HEADS:(j + 2) * PAD_HEADS, :].astype(jnp.bfloat16)
                qp = jnp.concatenate([jnp.concatenate([q0, zeros], axis=1), jnp.concatenate([zeros, q1], axis=1)], axis=0)
                kp = jnp.concatenate([kbuf[slot, j], kbuf[slot, j + 1]], axis=1)
                scores.append(lax.dot_general(qp, kp, (((1,), (1,)), ((), ())), preferred_element_type=jnp.float32))
            probs = []
            for i, j in enumerate(pairs):
                b = block * SLOT_ROWS + j
                limit = jnp.where(second, lens[b + 1], lens[b])
                s = jnp.where(col_pos <= limit, scores[i] * HEAD ** -0.5, -jnp.inf)
                e = jnp.exp(s - jnp.max(s, axis=-1, keepdims=True))
                probs.append((e.astype(jnp.bfloat16), jnp.sum(e, axis=-1, keepdims=True)))
            for i, j in enumerate(pairs):
                e, total = probs[i]
                vp = jnp.concatenate([vbuf[slot, j], vbuf[slot, j + 1]], axis=1)
                o = jnp.dot(e, vp, preferred_element_type=jnp.float32)
                at = (half * SLOT_ROWS + j) * PAD_HEADS
                os[at:at + PAD_HEADS, :] = o[:PAD_HEADS, :HEAD] / total[:PAD_HEADS]
                os[at + PAD_HEADS:at + 2 * PAD_HEADS, :] = o[PAD_HEADS:, HEAD:] / total[PAD_HEADS:]
            for move in moves(block, slot, False):
                move.start()

            @pl.when(block + AHEAD < blocks)
            def _():
                later = lax.rem(block + AHEAD, SLOTS)

                @pl.when(block + AHEAD >= SLOTS)
                def _():
                    for move in moves(block + AHEAD - SLOTS, later, False):
                        move.wait()
                for move in moves(block + AHEAD, later, True):
                    move.start()
        for h in range(heads):
            out_ref[pl.ds(pl.multiple_of(step * 16, 16), 16), h * HEAD:(h + 1) * HEAD] = os[pl.ds(h, 16, stride=PAD_HEADS), :].astype(jnp.bfloat16)

        @pl.when(step > 0)
        def _():
            put_out(step - 1).wait()
        put_out(step).start()

    put_out(blocks // 2 - 1).wait()
    for block in range(blocks - SLOTS, blocks):
        for move in moves(block, block % SLOTS, False):
            move.wait()


def attend(lens, q, k_new, v_new, k_cache, v_cache):
    rows, seq, kv, _ = k_cache.shape
    flat = seq * kv
    kc = k_cache.reshape(rows, flat, HEAD)
    vc = v_cache.reshape(rows, flat, HEAD)
    hbm = pl.BlockSpec(memory_space=pltpu.HBM)
    ko, vo, out = pl.pallas_call(
        attend_kernel,
        out_shape=(jax.ShapeDtypeStruct(kc.shape, kc.dtype), jax.ShapeDtypeStruct(vc.shape, vc.dtype), jax.ShapeDtypeStruct(q.shape, jnp.bfloat16)),
        in_specs=[hbm] * 6,
        out_specs=(hbm, hbm, hbm),
        scratch_shapes=[
            pltpu.VMEM((SLOTS, SLOT_ROWS, flat, HEAD), jnp.bfloat16),
            pltpu.VMEM((SLOTS, SLOT_ROWS, flat, HEAD), jnp.bfloat16),
            pltpu.VMEM(q.shape, q.dtype),
            pltpu.VMEM(k_new.shape, k_new.dtype),
            pltpu.VMEM(v_new.shape, v_new.dtype),
            pltpu.VMEM(q.shape, jnp.bfloat16),
            pltpu.VMEM((SLOT_ROWS * PAD_HEADS, HEAD), jnp.float32),
            pltpu.VMEM((2 * SLOT_ROWS * PAD_HEADS, HEAD), jnp.float32),
            pltpu.SemaphoreType.DMA((4, SLOTS)),
            pltpu.SemaphoreType.DMA((4,)),
            pltpu.SemaphoreType.DMA(()),
            pltpu.SMEM(lens.shape, lens.dtype),
        ],
        compiler_params=pltpu.CompilerParams(vmem_limit_bytes=67043328),
        name="attend",
    )(lens, q, k_new, v_new, kc, vc)
    return ko.reshape(k_cache.shape), vo.reshape(v_cache.shape), out


def tail_kernel(attn_hbm, x_hbm, gain_hbm, wo_hbm, wg_hbm, wu_hbm, wd_hbm, out_ref,
                attn_all, xown, wo_v, wd_v, ring, sb, rb, keep, mall, hbuf, gsend, grecv, act, ssq, ssr,
                wo_sem, wd_sem, ring_sem, x_sem, ici_ss, ici_rs, gu_ss, gu_rs, act_ss, act_rs, st_ss, st_rs, at_ss, at_rs, at_sem, gain_ref, gain_sem):
    my, mx = lax.axis_index("my"), lax.axis_index("mx")
    row_count, hidden = out_ref.shape
    half_rows = row_count // 2
    sub = half_rows // CHUNKS
    ff = wg_hbm.shape[1]
    steps = (ff // 128 + 1) // 2 * 128 // TILE
    own_w = steps * TILE
    shift = ff - own_w
    per_chunk = 2 * steps
    total_steps = CHUNKS * per_chunk

    def chunk_of(r):
        return lax.rem(my // 2 + r // 2, 2) * 2 + lax.rem(lax.rem(my, 2) + r % 2, 2)

    def device(r):
        return (chunk_of(r), mx)

    partner = (my, 1 - mx)
    first = lambda s: 1 if s == 0 else 2
    second = lambda s: 2 if s == 0 else 1

    def cols(r):
        return pl.ds(pl.multiple_of(chunk_of(r) * PIECE, 128), PIECE)

    barrier = pltpu.get_barrier_semaphore()
    for peer in (device(1), device(2), partner):
        pl.semaphore_signal(barrier, inc=1, device_id=peer, device_id_type=MESH)

    attn_copy = pltpu.make_async_copy(attn_hbm, attn_all.at[mx], at_sem)
    attn_copy.start()
    order = (3, 1, 2, 0)
    wo_copies = {r: pltpu.make_async_copy(wo_hbm.at[:, cols(r)], wo_v.at[:, pl.ds(i * PIECE, PIECE)], wo_sem.at[r]) for i, r in enumerate(order)}
    wd_copies = {r: pltpu.make_async_copy(wd_hbm.at[:, cols(r)], wd_v.at[:, pl.ds(i * PIECE, PIECE)], wd_sem.at[r]) for i, r in enumerate(order)}
    x_copy = pltpu.make_async_copy(x_hbm.at[:, cols(0)], xown, x_sem)
    for r in order:
        wo_copies[r].start()
    x_copy.start()
    gain_copy = pltpu.make_async_copy(gain_hbm, gain_ref, gain_sem)
    gain_copy.start()

    def ring_copies(g):
        slot = lax.rem(g, RING)
        at = lax.rem(g, per_chunk)
        mine = at // steps
        side = mine * mx + (1 - mine) * (1 - mx)
        col = pl.multiple_of(side * shift + lax.rem(at, steps) * TILE, 128)
        return (pltpu.make_async_copy(wg_hbm.at[:, pl.ds(col, TILE)], ring.at[slot, :, pl.ds(0, TILE)], ring_sem.at[slot, 0]),
                pltpu.make_async_copy(wu_hbm.at[:, pl.ds(col, TILE)], ring.at[slot, :, pl.ds(TILE, TILE)], ring_sem.at[slot, 1]))

    def remote(src, dst, ss, rs, peer):
        return pltpu.make_async_remote_copy(src_ref=src, dst_ref=dst, send_sem=ss, recv_sem=rs, device_id=peer, device_id_type=MESH)

    def hop(c, s, msg, src, dst, r):
        return remote(src, dst, ici_ss.at[c, s, msg], ici_rs.at[c, s, msg], device(r))

    attn_copy.wait()
    pl.semaphore_wait(barrier, 3)
    attn_msg = remote(attn_all.at[mx], attn_all.at[mx], at_ss, at_rs, partner)
    attn_msg.start()

    def for_rows(count, body, step=ROWS_STEP):
        @pl.loop(0, count // step)
        def _(i):
            body(pl.multiple_of(i * step, step))

    part = sub // 2

    def rs_msg(c, s, base, k):
        if k < 2:
            return hop(c, s, base + k, sb.at[c, s, k], rb.at[c, s, k], first(s))
        rows = pl.ds((k - 2) * part, part)
        return hop(c, s, base + k, sb.at[c, s, 2, rows], rb.at[c, s, 2, rows], second(s))

    def product(c, lhs, weights, copies, base, send):
        waited = []
        for lo in range(0, hidden, 2 * TILE):
            hi = lo + 2 * TILE
            held = [(i, order[i]) for i in range(4) if i * PIECE < hi and (i + 1) * PIECE > lo]
            for _, r in held:
                if copies and r not in waited:
                    waited.append(r)
                    copies[r].wait()
            acc = jnp.dot(lhs, weights[:, lo:hi], preferred_element_type=jnp.float32)
            for i, r in held:
                left, right = max(lo, i * PIECE), min(hi, (i + 1) * PIECE)
                where = slice(left - i * PIECE, right - i * PIECE)
                for s in range(2):
                    piece = acc[s * sub:(s + 1) * sub, left - lo:right - lo]
                    if r == 3 or r == first(s):
                        which = 0 if r == 3 else 1
                        sb[c, s, which, :, where] = piece.astype(jnp.bfloat16)
                        if send and right == (i + 1) * PIECE:
                            rs_msg(c, s, base, which).start()
                    else:
                        keep[c, s, 0 if r == second(s) else 1, :, where] = piece

    def rs_middle(c, base):
        for k in range(2):
            for s in range(2):
                if k == 0:
                    rs_msg(c, s, base, 0).wait_recv()

                def add(at, s=s, k=k):
                    rows = pl.ds(k * part + at, ROWS_STEP)
                    sb[c, s, 2, rows, :] = (keep[c, s, 0, rows, :] + rb[c, s, 0, rows, :].astype(jnp.float32)).astype(jnp.bfloat16)
                for_rows(part, add)
                rs_msg(c, s, base, 2 + k).start()

    def mid_at(c, s, r, k):
        return mall.at[c, chunk_of(r), pl.ds(s * sub + k * part, part), :]

    def out_at(c, s, r, k):
        return out_ref.at[pl.ds(s * half_rows + c * sub + k * part, part), cols(r)]

    def ag_msg(c, s, base, at, j, k):
        src = at(c, s, second(s) if j == 2 else 0, k)
        return hop(c, s, base + 2 * j + k, src, src, second(s) if j == 0 else first(s))

    def finish(c, base, store, at):
        for k in range(2):
            for s in range(2):
                if k == 0:
                    rs_msg(c, s, base, 1).wait_recv()
                rs_msg(c, s, base, 2 + k).wait_recv()

                def add(start, s=s, k=k):
                    rows = pl.ds(k * part + start, ROWS_STEP)
                    total = keep[c, s, 1, rows, :] + rb[c, s, 1, rows, :].astype(jnp.float32) + rb[c, s, 2, rows, :].astype(jnp.float32)
                    store(c, s, k * part + start, total)
                for_rows(part, add)
                ag_msg(c, s, base + 4, at, 0, k).start()
        for k in range(2):
            for s in range(2):
                ag_msg(c, s, base + 4, at, 1, k).start()

    def store_mid(c, s, at, total):
        total = total + xown[pl.ds(s * half_rows + c * sub + at, ROWS_STEP), :].astype(jnp.float32)
        mall[c, my, pl.ds(s * sub + at, ROWS_STEP), :] = total.astype(jnp.bfloat16)

    def store_out(c, s, at, total):
        total = total + mall[c, my, pl.ds(s * sub + at, ROWS_STEP), :].astype(jnp.float32)
        out_ref[pl.ds(s * half_rows + c * sub + at, ROWS_STEP), cols(0)] = total.astype(jnp.bfloat16)

    def finish_mid(c):
        finish(c, 0, store_mid, mid_at)

    def finish_out(c):
        finish(c, 10, store_out, out_at)

    def forward(c, base, at):
        for k in range(2):
            for s in range(2):
                ag_msg(c, s, base, at, 0, k).wait_recv()
                ag_msg(c, s, base, at, 2, k).start()

    def arrive(c, base, at):
        for s in range(2):
            for k in range(2):
                ag_msg(c, s, base, at, 1, k).wait_recv()
                ag_msg(c, s, base, at, 2, k).wait_recv()

    def sent(c, base, at=None):
        for s in range(2):
            if at is None:
                for k in range(4):
                    rs_msg(c, s, base, k).wait_send()
            else:
                for j in range(3):
                    for k in range(2):
                        ag_msg(c, s, base, at, j, k).wait_send()

    def normalise(c):
        def squares(at):
            rows = pl.ds(at, NORM_ROWS)
            total = jnp.zeros((NORM_ROWS, 128), jnp.float32)
            for j in range(4):
                for k in range(0, PIECE, 128):
                    m = mall[c, j, rows, k:k + 128].astype(jnp.float32)
                    total = total + m * m
            ssq[c, rows, :] = total
        for_rows(2 * sub, squares, NORM_ROWS)
        msg = remote(ssq.at[c], ssr.at[c], st_ss.at[c], st_rs.at[c], partner)
        msg.start()
        msg.wait()

        def scale(at):
            rows = pl.ds(at, NORM_ROWS)
            total = jnp.sum(ssq[c, rows, :] + ssr[c, rows, :], axis=1, keepdims=True)
            inv = lax.rsqrt(total / (2 * hidden) + NORM_EPS)
            for j in range(4):
                for k in range(PIECE // 128):
                    tile = j * (PIECE // 128) + k
                    m = mall[c, j, rows, k * 128:(k + 1) * 128].astype(jnp.float32)
                    hbuf[rows, tile * 128:(tile + 1) * 128] = (m * inv * gain_ref[tile:tile + 1, :].astype(jnp.float32)).astype(jnp.bfloat16)
        for_rows(2 * sub, scale, NORM_ROWS)

    def gu_msg(c, t):
        return remote(gsend.at[t], grecv.at[t], gu_ss.at[c, t], gu_rs.at[c, t], partner)

    def tiles(c, mine, lo, hi):
        @pl.loop(lo, hi)
        def _(t):
            g = c * per_chunk + mine * steps + t
            slot = lax.rem(g, RING)
            for copy in ring_copies(g):
                copy.wait()
            if mine:
                gu_msg(c, t).wait_recv()
            acc = jnp.dot(hbuf[...], ring[slot], preferred_element_type=jnp.float32)
            if mine:
                both = acc + grecv[t].astype(jnp.float32)
                gate, up = both[:, :TILE], both[:, TILE:]
                act[:, pl.ds(pl.multiple_of(mx * shift + t * TILE, 128), TILE)] = (gate * jax.nn.sigmoid(gate) * up).astype(jnp.bfloat16)
            else:
                gsend[t] = acc.astype(jnp.bfloat16)
            if not mine:
                gu_msg(c, t).start()

            @pl.when(g + RING < total_steps)
            def _():
                for copy in ring_copies(g + RING):
                    copy.start()

    cut = 3 * TILE

    def act_msg(c, k):
        width = cut if k == 0 else shift - cut
        where = pl.ds(pl.multiple_of(mx * own_w + (0 if k == 0 else cut), 128), width)
        return remote(act.at[:, where], act.at[:, where], act_ss.at[c, k], act_rs.at[c, k], partner)

    def gates_sent(c):
        for t in range(steps):
            gu_msg(c, t).wait_send()

    def attn_lhs(c):
        rows = slice(c * sub, (c + 1) * sub)
        return jnp.concatenate([attn_all[0, rows, :], attn_all[1, rows, :]], axis=0)

    def mlp(c, at, early, late):
        events = sorted([(at[0], 0, early), (at[1], 1, late), (steps + 4, 2, lambda: act_msg(c, 0).start()), (steps, 3, lambda: None), (per_chunk, 4, lambda: None)], key=lambda e: e[:2])
        done = 0
        for pos, _, act_on in events:
            if pos > done:
                mine = done // steps
                tiles(c, mine, done - mine * steps, pos - mine * steps)
                done = pos
            act_on()
        act_msg(c, 1).start()

    attn_msg.wait_recv()
    product(0, attn_lhs(0), wo_v, wo_copies, 0, True)
    for g in range(RING):
        for copy in ring_copies(g):
            copy.start()
    product(1, attn_lhs(1), wo_v, {}, 0, False)
    x_copy.wait()
    gain_copy.wait()
    for r in order:
        wd_copies[r].start()
    rs_middle(0, 0)
    for s in range(2):
        rs_msg(1, s, 0, 0).start()
    finish_mid(0)
    forward(0, 4, mid_at)
    rs_middle(1, 0)
    for s in range(2):
        rs_msg(1, s, 0, 1).start()
    arrive(0, 4, mid_at)
    normalise(0)
    mlp(0, SERVE[0], lambda: finish_mid(1), lambda: forward(1, 4, mid_at))
    sent(0, 0)
    for k in range(2):
        act_msg(0, k).wait_recv()
    product(0, act[...], wd_v, wd_copies, 10, True)
    gates_sent(0)
    for k in range(2):
        act_msg(0, k).wait_send()
    arrive(1, 4, mid_at)
    normalise(1)
    rs_middle(0, 10)
    mlp(1, SERVE[1], lambda: finish_out(0), lambda: forward(0, 14, out_at))
    sent(1, 0)
    for k in range(2):
        act_msg(1, k).wait_recv()
    product(1, act[...], wd_v, {}, 10, True)
    rs_middle(1, 10)
    arrive(0, 14, out_at)
    finish_out(1)
    forward(1, 14, out_at)
    gates_sent(1)
    for c in range(CHUNKS):
        sent(c, 4, mid_at)
        sent(c, 10)
        if c == 0:
            sent(c, 14, out_at)
    for k in range(2):
        act_msg(1, k).wait_send()
    attn_msg.wait_send()
    arrive(1, 14, out_at)
    sent(1, 14, out_at)


def tail(attn, x_in, gain, w_o, w_gate, w_up, w_down):
    rows, hidden = x_in.shape
    q_width = w_o.shape[0]
    ff = w_gate.shape[1]
    sub = rows // 2 // CHUNKS
    steps = (ff // 128 + 1) // 2 * 128 // TILE
    whole = pl.BlockSpec(memory_space=pltpu.VMEM)
    hbm = pl.BlockSpec(memory_space=pltpu.HBM)
    bf16, f32 = jnp.bfloat16, jnp.float32
    dma = pltpu.SemaphoreType.DMA
    return pl.pallas_call(
        tail_kernel,
        out_shape=jax.ShapeDtypeStruct((rows, hidden), bf16),
        in_specs=[hbm] * 7,
        out_specs=whole,
        scratch_shapes=[
            pltpu.VMEM((2, rows // 2, q_width), bf16),
            pltpu.VMEM((rows, PIECE), bf16),
            pltpu.VMEM((q_width, hidden), bf16),
            pltpu.VMEM((ff, hidden), bf16),
            pltpu.VMEM((RING, hidden, 2 * TILE), bf16),
            pltpu.VMEM((CHUNKS, 2, 3, sub, PIECE), bf16),
            pltpu.VMEM((CHUNKS, 2, 3, sub, PIECE), bf16),
            pltpu.VMEM((CHUNKS, 2, 2, sub, PIECE), f32),
            pltpu.VMEM((CHUNKS, 4, 2 * sub, PIECE), bf16),
            pltpu.VMEM((2 * sub, hidden), bf16),
            pltpu.VMEM((steps, 2 * sub, 2 * TILE), bf16),
            pltpu.VMEM((steps, 2 * sub, 2 * TILE), bf16),
            pltpu.VMEM((2 * sub, ff), bf16),
            pltpu.VMEM((CHUNKS, 2 * sub, 128), f32),
            pltpu.VMEM((CHUNKS, 2 * sub, 128), f32),
            dma((4,)), dma((4,)), dma((RING, 2)), dma(()),
            dma((CHUNKS, 2, 20)), dma((CHUNKS, 2, 20)),
            dma((CHUNKS, steps)), dma((CHUNKS, steps)),
            dma((CHUNKS, 2)), dma((CHUNKS, 2)),
            dma((CHUNKS,)), dma((CHUNKS,)),
            dma(()), dma(()), dma(()),
            pltpu.VMEM(gain.shape, bf16), dma(()),
        ],
        compiler_params=pltpu.CompilerParams(collective_id=1, has_side_effects=True, vmem_limit_bytes=67043328),
        name="tail",
    )(attn, x_in, gain, w_o, w_gate, w_up, w_down)


def head_kernel(lens_hbm, x_hbm, gain_hbm, bq_hbm, bk_hbm, bv_hbm, wq_hbm, wk_hbm, wv_hbm, q_out, k_out, v_out,
                xv, wv_all, hbuf, keep, psend, precv, ssq, ssr, cos_ref, sin_ref, x_sem, w_sem, st_ss, st_rs, p_ss, p_rs, lens, gain_ref, bq_ref, bk_ref, bv_ref, small_sem):
    my, mx = lax.axis_index("my"), lax.axis_index("mx")
    rows, hidden = xv.shape
    half = rows // 2
    q_cols, kv_cols = wq_hbm.shape[1], wk_hbm.shape[1]
    width = q_cols + 2 * kv_cols
    partner = (my, 1 - mx)
    barrier = pltpu.get_barrier_semaphore()
    pl.semaphore_signal(barrier, inc=1, device_id=partner, device_id_type=MESH)

    x_parts = 4
    x_rows = rows // x_parts
    x_copies = [pltpu.make_async_copy(x_hbm.at[pl.ds(i * x_rows, x_rows)], xv.at[pl.ds(i * x_rows, x_rows)], x_sem.at[i]) for i in range(x_parts)]
    w_copies = [
        pltpu.make_async_copy(wq_hbm, wv_all.at[:, pl.ds(0, q_cols)], w_sem.at[0]),
        pltpu.make_async_copy(wk_hbm, wv_all.at[:, pl.ds(q_cols, kv_cols)], w_sem.at[1]),
        pltpu.make_async_copy(wv_hbm, wv_all.at[:, pl.ds(q_cols + kv_cols, kv_cols)], w_sem.at[2]),
    ]
    small = [pltpu.make_async_copy(src, dst, small_sem.at[i]) for i, (src, dst) in enumerate(((lens_hbm, lens), (gain_hbm, gain_ref), (bq_hbm, bq_ref), (bk_hbm, bk_ref), (bv_hbm, bv_ref)))]
    for copy in x_copies + small:
        copy.start()

    def remote(src, dst, ss, rs):
        return pltpu.make_async_remote_copy(src_ref=src, dst_ref=dst, send_sem=ss, recv_sem=rs, device_id=partner, device_id_type=MESH)

    for i in range(x_parts):
        x_copies[i].wait()
        if i == x_parts - 1:
            for copy in w_copies:
                copy.start()

        @pl.loop(0, x_rows // HEAD_ROWS)
        def _(step, i=i):
            at = pl.ds(pl.multiple_of(i * x_rows + step * HEAD_ROWS, HEAD_ROWS), HEAD_ROWS)
            total = jnp.zeros((HEAD_ROWS, 128), jnp.float32)
            for k in range(0, hidden, 128):
                m = xv[at, k:k + 128].astype(jnp.float32)
                total = total + m * m
            ssq[at, :] = total
    pl.semaphore_wait(barrier, 1)
    stats = remote(ssq, ssr, st_ss, st_rs)
    stats.start()
    for copy in small:
        copy.wait()
    row_of = lax.broadcasted_iota(jnp.int32, (ROWS_STEP, HEAD), 0)
    lane = lax.broadcasted_iota(jnp.int32, (ROWS_STEP, HEAD), 1)
    lower = lane < HEAD // 2
    freq = jnp.exp(lax.rem(lane, HEAD // 2).astype(jnp.float32) * (-2.0 * math.log(ROPE_THETA) / HEAD))

    @pl.loop(0, half // ROWS_STEP)
    def _(step):
        start = pl.multiple_of(step * ROWS_STEP, ROWS_STEP)
        pos = jnp.zeros((ROWS_STEP, HEAD), jnp.int32)
        for i in range(ROWS_STEP):
            pos = jnp.where(row_of == i, lens[start + i], pos)
        angles = pos.astype(jnp.float32) * freq
        cos_ref[pl.ds(start, ROWS_STEP), :] = jnp.cos(angles)
        sin = jnp.sin(angles)
        sin_ref[pl.ds(start, ROWS_STEP), :] = jnp.where(lower, -sin, sin)

    stats.wait()

    def normalise(start):
        @pl.loop(0, half // NORM_ROWS)
        def _(step):
            at = pl.ds(pl.multiple_of(start + step * NORM_ROWS, NORM_ROWS), NORM_ROWS)
            total = jnp.sum(ssq[at, :] + ssr[at, :], axis=1, keepdims=True)
            inv = lax.rsqrt(total / (2 * hidden) + NORM_EPS)
            for k in range(hidden // 128):
                lanes = slice(k * 128, (k + 1) * 128)
                hbuf[at, lanes] = (xv[at, lanes].astype(jnp.float32) * inv * gain_ref[k:k + 1, :].astype(jnp.float32)).astype(jnp.bfloat16)

    theirs = pl.multiple_of((1 - mx) * half, half)
    mine = pl.multiple_of(mx * half, half)
    normalise(theirs)
    for copy in w_copies:
        copy.wait()
    spans = [(lo, min(lo + 512, width)) for lo in range(0, width, 512)]

    def piece(i, lo, hi):
        return remote(psend.at[:, pl.ds(lo, hi - lo)], precv.at[:, pl.ds(lo, hi - lo)], p_ss.at[i], p_rs.at[i])

    for i, (lo, hi) in enumerate(spans):
        psend[:, lo:hi] = jnp.dot(hbuf[pl.ds(theirs, half), :], wv_all[:, lo:hi], preferred_element_type=jnp.float32).astype(jnp.bfloat16)
        piece(i, lo, hi).start()
    normalise(mine)
    for i, (lo, hi) in enumerate(spans):
        keep[:, lo:hi] = jnp.dot(hbuf[pl.ds(mine, half), :], wv_all[:, lo:hi], preferred_element_type=jnp.float32)
    for i, (lo, hi) in enumerate(spans):
        piece(i, lo, hi).wait_recv()

    def bias_row(ref, h):
        return ref[h:h + 1, :].astype(jnp.float32)

    @pl.loop(0, half // ROWS_STEP)
    def _(step):
        at = pl.ds(pl.multiple_of(step * ROWS_STEP, ROWS_STEP), ROWS_STEP)
        cos_tab, sin_tab = cos_ref[at, :], sin_ref[at, :]
        for h in range(width // HEAD):
            lanes = slice(h * HEAD, (h + 1) * HEAD)
            vals = keep[at, lanes] + precv[at, lanes].astype(jnp.float32)
            if h < q_cols // HEAD:
                out, ref, j, spin = q_out, bq_ref, h, True
            elif h < (q_cols + kv_cols) // HEAD:
                out, ref, j, spin = k_out, bk_ref, h - q_cols // HEAD, True
            else:
                out, ref, j, spin = v_out, bv_ref, h - (q_cols + kv_cols) // HEAD, False
            vals = vals + bias_row(ref, j)
            if spin:
                vals = vals * cos_tab + pltpu.roll(vals, HEAD // 2, 1) * sin_tab
            out[at, j * HEAD:(j + 1) * HEAD] = vals.astype(jnp.bfloat16).astype(jnp.float32)

    for i, (lo, hi) in enumerate(spans):
        piece(i, lo, hi).wait_send()


def head(lens, x_in, gain, b_q, b_k, b_v, w_q, w_k, w_v):
    rows, hidden = x_in.shape
    half = rows // 2
    q_cols, kv_cols = w_q.shape[1], w_k.shape[1]
    width = q_cols + 2 * kv_cols
    whole = pl.BlockSpec(memory_space=pltpu.VMEM)
    hbm = pl.BlockSpec(memory_space=pltpu.HBM)
    bf16, f32 = jnp.bfloat16, jnp.float32
    dma = pltpu.SemaphoreType.DMA
    return pl.pallas_call(
        head_kernel,
        out_shape=(jax.ShapeDtypeStruct((half, q_cols), f32), jax.ShapeDtypeStruct((half, kv_cols), f32), jax.ShapeDtypeStruct((half, kv_cols), f32)),
        in_specs=[hbm] * 9,
        out_specs=(whole, whole, whole),
        scratch_shapes=[
            pltpu.VMEM((rows, hidden), bf16),
            pltpu.VMEM((hidden, width), bf16),
            pltpu.VMEM((rows, hidden), bf16),
            pltpu.VMEM((half, width), f32),
            pltpu.VMEM((half, width), bf16),
            pltpu.VMEM((half, width), bf16),
            pltpu.VMEM((rows, 128), f32),
            pltpu.VMEM((rows, 128), f32),
            pltpu.VMEM((half, HEAD), f32),
            pltpu.VMEM((half, HEAD), f32),
            dma((4,)), dma((3,)), dma(()), dma(()), dma((4,)), dma((4,)),
            pltpu.SMEM(lens.shape, lens.dtype),
            pltpu.VMEM(gain.shape, bf16), pltpu.VMEM(b_q.shape, bf16), pltpu.VMEM(b_k.shape, bf16), pltpu.VMEM(b_v.shape, bf16),
            dma((5,)),
        ],
        compiler_params=pltpu.CompilerParams(collective_id=0, has_side_effects=True, vmem_limit_bytes=67043328),
        name="head",
    )(lens, x_in, gain, b_q, b_k, b_v, w_q, w_k, w_v)


def lanes_of(vec):
    return vec.reshape(-1, 128)


def solution(mesh):
    act_spec = P(None, "mx")
    cache_spec = P("mx", None, "my", None)
    in_specs = (act_spec, P("mx"), P("mx"), P("mx"), P("mx", "my"), P("my"), P("mx", "my"), P("my"), P("mx", "my"), P("my"), P("my", "mx"), P("mx", "my"), P("mx", "my"), P("my", "mx"), cache_spec, cache_spec)
    out_specs = (act_spec, cache_spec, cache_spec)

    def local_layer(x_in, seq_lens, gain_attn, gain_mlp, w_q, b_q, w_k, b_k, w_v, b_v, w_o, w_gate, w_up, w_down, k_cache, v_cache):
        q_rot, k_rot, v_new = head(seq_lens, x_in, lanes_of(gain_attn), lanes_of(b_q), lanes_of(b_k), lanes_of(b_v), w_q, w_k, w_v)
        k_cache_out, v_cache_out, attn_rows = attend(seq_lens, q_rot, k_rot, v_new, k_cache, v_cache)
        x_out = tail(attn_rows, x_in, lanes_of(gain_mlp), w_o, w_gate, w_up, w_down)
        return x_out, k_cache_out, v_cache_out

    return jax.shard_map(local_layer, mesh=mesh, in_specs=in_specs, out_specs=out_specs, check_vma=False)
```
